32 devices in a mesh: chain: 8 (over y, x, core), par: 4 (over z).
Axes of the slice: x: 2, y: 2, z: 4, core: 2. Of those that a mesh axis runs over, the one named last changes fastest.
Arguments:
- propagation_gains: bfloat16 [4, 16, 64, 8192], P('par', None, None, 'chain'), may hold values from -0.13258252 to 0.13258252, as said below
- observed_samples: bfloat16 [4, 16, 32, 8192], P('par', None, None, 'chain'), may hold values from -6 to 6
- disturbance_variance: float32 [4, 16], P(None, 'chain'), may hold values from 0.05 to 0.5
- retained_branches: int32 [4, 16, 16, 1024], P(None, 'chain', 'par'), may hold values from 0 to 63
Outputs:
- distances: float32 [4, 16, 16, 1024], P(None, 'chain', 'par')
The draws below stay inside these ranges and needn't reach their ends.
Inputs may be any that keep to these rules, and one draw needn't show every extreme that they name: `propagation_gains`: row 2u holds the real and row 2u+1 the imaginary part of the channel to user u.
All inputs are finite; a program needn't handle non-finite values.
Results may differ from the reference program's by a relative error of at most 0.0003.
Values sent between devices are 32-bit elements; how exact they have to be, the bound alone decides.
A program may use at most 64 MiB of HBM per device.

```python
import math
import jax
import jax.numpy as jnp
from jax import lax

TERMINAL_NUMBER = 32
KEPT_BRANCHES = 32
FREQ_GROUP_NUM = 4
TONES_PER_GROUP = 16
SLOTS_PER_FRAME = 16
ANTENNA_TOTAL = 8192


def draw_propagation_gains(key, part):
    base = jax.random.fold_in(key, 11)
    private_key, common_key, key_gain = jax.random.split(base, 3)
    common_weight = 0.5
    gain_low = 0.5
    gain_high = 2.0
    private_part = jnp.clip(jax.random.normal(private_key, (FREQ_GROUP_NUM, TONES_PER_GROUP, 2 * TERMINAL_NUMBER, ANTENNA_TOTAL), jnp.float32), -4.0, 4.0)
    common_part = jnp.clip(jax.random.normal(common_key, (FREQ_GROUP_NUM, TONES_PER_GROUP, 2, ANTENNA_TOTAL), jnp.float32), -4.0, 4.0)
    shared = jnp.tile(common_part, (1, 1, TERMINAL_NUMBER, 1))
    log_gain = jax.random.uniform(key_gain, (FREQ_GROUP_NUM, TONES_PER_GROUP, TERMINAL_NUMBER, 1), jnp.float32, math.log(gain_low), math.log(gain_high))
    gains = jnp.repeat(jnp.exp(log_gain), 2, axis=2)
    factor_matrix = 1.0 / math.sqrt(2.0 * ANTENNA_TOTAL * (1.0 + common_weight * common_weight))
    return (gains * (private_part + common_weight * shared) * factor_matrix).astype(jnp.bfloat16)


def touch_ends(drawn, stream_key, least, high):
    longest = drawn.shape.index(max(drawn.shape))
    spots = []
    for shift in (0, 1):
        where = [jax.random.randint(jax.random.fold_in(stream_key, axis), (), 0, length) for axis, length in enumerate(drawn.shape)]
        where[longest] = (where[longest] + shift) % drawn.shape[longest]
        spots.append(tuple(where))
    return drawn.at[spots[0]].set(least).at[spots[1]].set(high)


def levels(own_key, dims, cuts, least, high):
    def one(dim, shards_of):
        heights = jax.random.uniform(jax.random.fold_in(jax.random.fold_in(own_key, 6), dim), (shards_of,), jnp.float32, least / len(cuts), high / len(cuts))
        return jnp.repeat(jnp.exp(heights), dims[dim] // shards_of).reshape((-1,) + (1,) * (len(dims) - dim - 1))

    factor_of = one(*cuts[0])
    for cut in cuts[1:]:
        factor_of = factor_of * one(*cut)
    return factor_of


def scatter_about(stream_key, shape, deviation, bound, shards=(), kind=jnp.bfloat16):
    level = levels(stream_key, shape, shards, -0.22, 0.18) if shards else 1.0
    result = jax.random.normal(stream_key, shape, jnp.float32) * deviation * level
    return jnp.minimum(jnp.maximum(result, -bound), bound).astype(kind)


def setup_inputs(seed: int = 0) -> dict:
    keys = jax.random.split(jax.random.key(seed), 5)
    return {
        "propagation_gains": draw_propagation_gains(jax.random.fold_in(keys[4], 71), 0),
        "observed_samples": scatter_about(keys[1], (FREQ_GROUP_NUM, TONES_PER_GROUP, 2 * SLOTS_PER_FRAME, ANTENNA_TOTAL), 1.0, 6.0, ((0, 4), (3, 8))),
        "disturbance_variance": jnp.clip(jnp.exp(math.log(0.5) - 2.3025851 * jax.random.uniform(keys[2], (FREQ_GROUP_NUM, TONES_PER_GROUP), jnp.float32) ** levels(keys[2], (FREQ_GROUP_NUM, TONES_PER_GROUP), ((1, 8),), -0.2, 0.2)), 0.05, 0.5),
        "retained_branches": touch_ends(jax.random.randint(keys[3], (FREQ_GROUP_NUM, TONES_PER_GROUP, SLOTS_PER_FRAME, KEPT_BRANCHES * TERMINAL_NUMBER), 0, 64), jax.random.fold_in(keys[3], 1), 0, 63).astype(jnp.int32),
    }


constellation_norm = 1.0 / 42.0 ** 0.5

def fold_stats(raw_gram, raw_cross):
    outer_dimensions = raw_gram.shape[:-2]
    terminal_number = raw_gram.shape[-1] // 2
    pieces = raw_gram.reshape(outer_dimensions + (terminal_number, 2, terminal_number, 2))
    same_part = pieces[..., :, 0, :, 0] + pieces[..., :, 1, :, 1]
    cross_part = pieces[..., :, 1, :, 0] - pieces[..., :, 0, :, 1]
    crossed = raw_cross.reshape(outer_dimensions + (terminal_number, 2, -1, 2))
    rhs_real = crossed[..., :, 0, :, 0] + crossed[..., :, 1, :, 1]
    rhs_imag = crossed[..., :, 0, :, 1] - crossed[..., :, 1, :, 0]
    rhs = jnp.stack([rhs_real, rhs_imag], axis=-2).reshape(outer_dimensions + (2 * terminal_number, -1))
    return (same_part, cross_part, rhs)

def assemble(same_part, cross_part, noise):
    row_even = jnp.stack([same_part, cross_part], axis=-1)
    row_odd = jnp.stack([-cross_part, same_part], axis=-1)
    whole = jnp.stack([row_even, row_odd], axis=-3)
    order = 2 * same_part.shape[-1]
    gram = whole.reshape(same_part.shape[:-2] + (order, order))
    return gram + noise[..., None, None] * jnp.eye(order, dtype=jnp.float32)

def estimate_transmitted(cholesky_triangle, whitened_observation, retained_branches):
    terminal_number = cholesky_triangle.shape[-1] // 2
    outer_dimensions = retained_branches.shape[:-1]
    kept_branch_number = retained_branches.shape[-1] // terminal_number
    constellation_position = retained_branches.reshape(outer_dimensions + (kept_branch_number, terminal_number))
    inphase_amplitude = (2 * (constellation_position % 8) - 7).astype(jnp.float32)
    quadrature_amplitude = (2 * (constellation_position // 8) - 7).astype(jnp.float32)
    branch_vector = jnp.stack([inphase_amplitude, quadrature_amplitude], axis=-1).reshape(outer_dimensions + (kept_branch_number, 2 * terminal_number)) * constellation_norm
    upper_factor = jnp.swapaxes(cholesky_triangle, -1, -2)
    mapped = jnp.einsum('bsij,bstkj->bstki', upper_factor, branch_vector, precision=lax.Precision.HIGHEST)
    remainder_error = jnp.swapaxes(whitened_observation, -1, -2)[..., None, :] - mapped
    squared_errors = (remainder_error * remainder_error).reshape(outer_dimensions + (kept_branch_number, terminal_number, 2)).sum(axis=-1)
    accrued_metric = jnp.cumsum(squared_errors[..., ::-1], axis=-1)[..., ::-1] / terminal_number
    return accrued_metric.reshape(outer_dimensions + (kept_branch_number * terminal_number,))

def reference(propagation_gains, observed_samples, disturbance_variance, retained_branches):

    def band_stats(inputs):
        chan_band, recv_band = inputs
        chan_f = chan_band.astype(jnp.float32)
        recv_f = recv_band.astype(jnp.float32)
        gram_band = jnp.einsum('sra,sqa->srq', chan_f, chan_f, precision=lax.Precision.HIGHEST)
        cross_band = jnp.einsum('sra,sqa->srq', chan_f, recv_f, precision=lax.Precision.HIGHEST)
        return (gram_band, cross_band)
    raw_gram, raw_cross = lax.map(band_stats, (propagation_gains, observed_samples))
    same_part, cross_part, rhs = fold_stats(raw_gram, raw_cross)
    gram = assemble(same_part, cross_part, disturbance_variance)
    cholesky_triangle = jnp.linalg.cholesky(gram)
    whitened_observation = jax.scipy.linalg.solve_triangular(cholesky_triangle, rhs, lower=True)
    return estimate_transmitted(cholesky_triangle, whitened_observation, retained_branches)
```

```python
import functools
import jax
import jax.numpy as jnp
from jax import lax
from jax.experimental import pallas as pl
from jax.experimental.pallas import tpu as pltpu
from jax.sharding import PartitionSpec as P

constellation_norm = 1.0 / 42.0**0.5
LANES = 128
PANEL = 4
MESH = pl.DeviceIdType.MESH
NT = (((1,), (1,)), ((), ()))


def iota(shape, dim):
    return lax.broadcasted_iota(jnp.int32, shape, dim)


def split(x):
    high = x.astype(jnp.bfloat16)
    return high, (x - high.astype(jnp.float32)).astype(jnp.bfloat16)


def pair_swap(x):
    even = iota(x.shape, 1) % 2 == 0
    return jnp.where(even, pltpu.roll(x, LANES - 1, 1), pltpu.roll(x, 1, 1))


def eliminate(mats, users):
    groups = users // 8
    blocks, turned = [], []
    for mat in mats:
        odd = iota((8, LANES), 1) % 2 == 1
        parts = [mat[8 * g : 8 * g + 8, :] for g in range(groups)]
        blocks.append(parts)
        turned.append([jnp.where(odd, pair_swap(p), -pair_swap(p)) for p in parts])
    row = iota((8, LANES), 0)
    for start in range(0, users, PANEL):
        home = start // 8
        panels = [
            [
                {g: jnp.broadcast_to(a[g][:, lane : lane + 1], (8, LANES)) for g in range(home, groups)}
                for lane in range(2 * start, 2 * (start + PANEL))
            ]
            for a in blocks
        ]
        for j in range(start, min(start + PANEL, users - 1)):
            at, c = j % 8, j - start
            for a, ia, panel in zip(blocks, turned, panels):
                real, imag = panel[2 * c], panel[2 * c + 1]
                inverse = 1.0 / real[home][at : at + 1, :]
                pivot_row = a[home][at : at + 1, :] * inverse
                turned_row = ia[home][at : at + 1, :] * inverse
                later = [
                    (d, real[home][at + d - c : at + d - c + 1, :] * inverse, imag[home][at + d - c : at + d - c + 1, :] * inverse)
                    for d in range(c + 1, PANEL)
                ]
                for g in range(home + (at == 7), groups):
                    fr, fi = real[g], imag[g]
                    if g == home:
                        fr, fi = jnp.where(row > at, fr, 0.0), jnp.where(row > at, fi, 0.0)
                    for d, x, y in later:
                        panel[2 * d][g] = panel[2 * d][g] - (fr * x + fi * y)
                        panel[2 * d + 1][g] = panel[2 * d + 1][g] - (fi * x - fr * y)
                    a[g] = a[g] - (fr * pivot_row + fi * turned_row)
                    ia[g] = ia[g] - (fr * turned_row - fi * pivot_row)
    lane, line = iota((users, LANES), 1), iota((users, LANES), 0)
    keep = (lane >= 2 * line) & (lane != 2 * line + 1) | (lane >= 2 * users)
    out = []
    for a in blocks:
        full = jnp.concatenate(a, axis=0)
        pivots = jnp.sum(jnp.where(lane == 2 * line, full, 0.0), axis=1, keepdims=True)
        out.append(jnp.where(keep, full * lax.rsqrt(pivots), 0.0))
    return out


def kernel(
    dims, noise_any, gains_ref, samples_ref, branches_any, out_ref,
    noise_ref, branches_ref, held, raw, part, came, points, packed, taken, rotations,
    small_sem, load_sem, send_sem, recv_sem, usend_sem, urecv_sem,
):
    clusters, bands, users, symbols, share, mine_t, pieces = dims
    copies = LANES // users
    lines = pieces * mine_t
    me, band = lax.axis_index("chain"), lax.axis_index("par")

    barrier = pltpu.get_barrier_semaphore()
    for k in range(1, clusters):
        pl.semaphore_signal(barrier, inc=1, device_id={"chain": lax.rem(me + k, clusters)}, device_id_type=MESH)
    for k in range(1, bands):
        pl.semaphore_signal(barrier, inc=1, device_id={"par": lax.rem(band + k, bands)}, device_id_type=MESH)

    order = list(range(1, clusters)) + [0]
    loads = {}
    for k in order:
        tones = pl.ds(lax.rem(me + k, clusters) * share, share)
        loads[k] = (
            pltpu.make_async_copy(
                gains_ref.at[0, tones], held.at[k, :, pl.ds(0, 2 * users)], load_sem.at[0, k]
            ),
            pltpu.make_async_copy(
                samples_ref.at[0, tones], held.at[k, :, pl.ds(2 * users, 2 * symbols)], load_sem.at[1, k]
            ),
        )
        for copy in loads[k]:
            copy.start()

    small = (
        pltpu.make_async_copy(noise_any, noise_ref, small_sem.at[0]),
        pltpu.make_async_copy(branches_any, branches_ref, small_sem.at[1]),
    )
    for copy in small:
        copy.start()
    raw[...] = jnp.zeros_like(raw)
    even = iota((users, LANES), 1) % 2 == 0
    sends = []
    for number, k in enumerate(order):
        for copy in loads[k]:
            copy.wait()
        for s in range(share):
            slot = (number * share + s) % raw.shape[0]
            both = held[k, s]
            raw[slot, :, : 2 * (users + symbols)] = lax.dot_general(
                both[: 2 * users], both, NT, preferred_element_type=jnp.float32
            )
            on_even = raw[slot, pl.ds(0, users, stride=2), :]
            on_odd = raw[slot, pl.ds(1, users, stride=2), :]
            part[k, s] = pair_swap(on_odd) + jnp.where(even, on_even, -on_even)
        if k:
            if number == 0:
                pl.semaphore_wait(barrier, clusters + bands - 2)
            copy = pltpu.make_async_remote_copy(
                src_ref=part.at[k], dst_ref=came.at[k], send_sem=send_sem.at[k], recv_sem=recv_sem.at[k],
                device_id={"chain": lax.rem(me + k, clusters)}, device_id_type=MESH,
            )
            copy.start()
            sends.append(copy)

    for copy in small:
        copy.wait()
    for b in range(bands):
        for s in range(share):
            q = jnp.concatenate(
                [branches_ref[b, s, :, LANES * r : LANES * (r + 1)] for r in range(pieces)], axis=0
            )
            points[b, s, :, :LANES] = (2 * (q & 7) - 7).astype(jnp.float32).astype(jnp.bfloat16)
            points[b, s, :, LANES:] = (2 * (q >> 3) - 7).astype(jnp.float32).astype(jnp.bfloat16)

    lane, line = iota((users, LANES), 1), iota((users, LANES), 0)
    noises = [
        jnp.sum(jnp.where(iota((1, bands), 1) == band, noise_ref[s : s + 1, :], 0.0), axis=1, keepdims=True)
        for s in range(share)
    ]
    totals = [part[0, s] for s in range(share)]
    for copy in sends:
        copy.wait_recv()
    for k in range(1, clusters):
        totals = [total + came[k, s] for s, total in enumerate(totals)]
    mats = [
        jnp.where(lane == 2 * line, total + noises[s], total) for s, total in enumerate(totals)
    ]
    factors = eliminate(mats, users)

    source, target = iota((LANES, LANES), 0), iota((LANES, LANES), 1) % (2 * users)
    spread = (source == 2 * (target % users) + target // users).astype(jnp.float32).astype(jnp.bfloat16)
    rows = 2 * mine_t
    r, c = iota((bands * rows, LANES), 0), iota((bands * rows, LANES), 1)
    is_odd = (r % rows) // mine_t
    wanted = 2 * users + 2 * ((r // rows) * mine_t + r % mine_t) + is_odd
    pick = jnp.where(c == wanted, (1 - 2 * is_odd).astype(jnp.float32), 0.0).astype(jnp.bfloat16)
    pick = jnp.concatenate([pick, pick], axis=1)
    half = users // 2
    left = iota((half, LANES), 1) < 2 * users
    for s, factor in enumerate(factors):
        high, low = split(factor * constellation_norm)
        wide = jnp.dot(high, spread, preferred_element_type=jnp.float32) + jnp.dot(
            low, spread, preferred_element_type=jnp.float32
        )
        folded = jnp.where(left, wide[:half], wide[half:])
        for k in range(bands):
            packed[k, s, :half] = folded
        high, low = split(factor)
        weights = jnp.concatenate(
            [jnp.concatenate([high] * copies, axis=0), jnp.concatenate([low] * copies, axis=0)], axis=1
        )
        rotations[s] = lax.dot_general(pick, weights, NT, preferred_element_type=jnp.float32)
        for k in range(bands):
            peer = lax.rem(band + k, bands)
            packed[k, s, half:] = rotations[s, pl.ds(pl.multiple_of(peer * rows, rows), rows), :]
    usends = []
    for k in range(1, bands):
        copy = pltpu.make_async_remote_copy(
            src_ref=packed.at[k], dst_ref=taken.at[k], send_sem=usend_sem.at[k], recv_sem=urecv_sem.at[k],
            device_id={"par": lax.rem(band + k, bands)}, device_id_type=MESH,
        )
        copy.start()
        usends.append(copy)

    sr, sc = iota((LANES, LANES), 0), iota((LANES, LANES), 1)
    suffix = jnp.where((sr // users == sc // users) & (sr >= sc), 1.0 / users, 0.0).astype(jnp.bfloat16)
    suffix = jnp.concatenate([suffix, suffix], axis=0)
    lane_block = lane // users
    for k in range(bands):
        if k:
            usends[k - 1].wait_recv()
        b = lax.rem(band + bands - k, bands)
        box = taken if k else packed
        for s in range(share):
            folded = box[k, s, :half]
            crossed = pltpu.roll(folded, 2 * users, 1)
            first = jnp.concatenate(
                [jnp.where(left, folded, crossed), jnp.where(left, crossed, folded)], axis=0
            )
            second = pltpu.roll(first, users, 1)
            ons, offs = [], []
            for i in range(copies):
                here = lane_block == i
                real, imag = (first, second) if i % 2 == 0 else (second, first)
                real, imag = jnp.where(here, real, 0.0), jnp.where(here, imag, 0.0)
                ons.append(jnp.concatenate([real, imag], axis=1))
                offs.append(jnp.concatenate([-imag, real], axis=1))
            high, low = split(jnp.concatenate(ons + offs, axis=0))
            p = points[b, s]
            mapped = lax.dot_general(p, high, NT, preferred_element_type=jnp.float32) + lax.dot_general(
                p, low, NT, preferred_element_type=jnp.float32
            )
            on = jnp.concatenate([box[k, s, half : half + mine_t]] * pieces, axis=0) - mapped[:, :LANES]
            off = jnp.concatenate([box[k, s, half + mine_t :]] * pieces, axis=0) - mapped[:, LANES:]
            high, low = split(on * on + off * off)
            result = jnp.dot(
                jnp.concatenate([high, low], axis=1), suffix, preferred_element_type=jnp.float32
            )
            for r in range(pieces):
                out_ref[b, s, :, LANES * r : LANES * (r + 1)] = result[mine_t * r : mine_t * (r + 1)]
    for copy in sends + usends:
        copy.wait_send()


def local(propagation_gains, observed_samples, disturbance_variance, retained_branches):
    clusters, bands = lax.axis_size("chain"), lax.axis_size("par")
    _, tones, double_users, antennas = propagation_gains.shape
    users, symbols = double_users // 2, observed_samples.shape[2] // 2
    share, mine_t = tones // clusters, symbols // bands
    pieces = retained_branches.shape[-1] // LANES
    dims = (clusters, bands, users, symbols, share, mine_t, pieces)
    f32, bf16 = jnp.float32, jnp.bfloat16
    vmem, dma = pltpu.VMEM, pltpu.SemaphoreType.DMA
    payload = users // 2 + 2 * mine_t
    return pl.pallas_call(
        functools.partial(kernel, dims),
        out_shape=pltpu.VMEM(retained_branches.shape, f32),
        in_specs=[
            pl.BlockSpec(memory_space=pl.ANY),
            pl.BlockSpec(memory_space=pl.ANY),
            pl.BlockSpec(memory_space=pl.ANY),
            pl.BlockSpec(memory_space=pl.ANY),
        ],
        out_specs=pl.BlockSpec(memory_space=pltpu.VMEM),
        scratch_shapes=[
            vmem(disturbance_variance.shape[::-1], f32),
            vmem(retained_branches.shape, jnp.int32),
            vmem((clusters, share, 2 * (users + symbols), antennas), bf16),
            vmem((4, 2 * users, LANES), f32),
            vmem((clusters, share, users, LANES), f32),
            vmem((clusters, share, users, LANES), f32),
            vmem((bands, share, pieces * mine_t, 2 * LANES), bf16),
            vmem((bands, share, payload, LANES), f32),
            vmem((bands, share, payload, LANES), f32),
            vmem((share, bands * 2 * mine_t, LANES), f32),
            dma((2,)), dma((2, clusters)), dma((clusters,)), dma((clusters,)), dma((bands,)), dma((bands,)),
        ],
        compiler_params=pltpu.CompilerParams(collective_id=0, has_side_effects=True),
        name="detect",
    )(*(
        pltpu.with_memory_space_constraint(x, pltpu.HBM)
        for x in (disturbance_variance.T, propagation_gains, observed_samples, retained_branches)
    ))


def solution(mesh):
    placed = (
        P("par", None, None, "chain"),
        P("par", None, None, "chain"),
        P(None, "chain"),
        P(None, "chain", "par", None),
    )
    return jax.shard_map(
        local, mesh=mesh, in_specs=placed, out_specs=P(None, "chain", "par", None), check_vma=False
    )
```

```python
import functools
import jax
import jax.numpy as jnp
from jax import lax
from jax.experimental import pallas as pl
from jax.experimental.pallas import tpu as pltpu
from jax.sharding import PartitionSpec as P

constellation_norm = 1.0 / 42.0**0.5
LANES = 128
PANEL = 4
MESH = pl.DeviceIdType.MESH
NT = (((1,), (1,)), ((), ()))


def iota(shape, dim):
    return lax.broadcasted_iota(jnp.int32, shape, dim)


def split(x):
    high = x.astype(jnp.bfloat16)
    return high, (x - high.astype(jnp.float32)).astype(jnp.bfloat16)


def pair_swap(x):
    even = iota(x.shape, 1) % 2 == 0
    return jnp.where(even, pltpu.roll(x, LANES - 1, 1), pltpu.roll(x, 1, 1))


def eliminate(mats, users):
    groups = users // 8
    blocks, turned = [], []
    for mat in mats:
        odd = iota((8, LANES), 1) % 2 == 1
        parts = [mat[8 * g : 8 * g + 8, :] for g in range(groups)]
        blocks.append(parts)
        turned.append([jnp.where(odd, pair_swap(p), -pair_swap(p)) for p in parts])
    row = iota((8, LANES), 0)
    for start in range(0, users, PANEL):
        home = start // 8
        panels = [
            [
                {g: jnp.broadcast_to(a[g][:, lane : lane + 1], (8, LANES)) for g in range(home, groups)}
                for lane in range(2 * start, 2 * (start + PANEL))
            ]
            for a in blocks
        ]
        for j in range(start, min(start + PANEL, users - 1)):
            at, c = j % 8, j - start
            for a, ia, panel in zip(blocks, turned, panels):
                real, imag = panel[2 * c], panel[2 * c + 1]
                inverse = 1.0 / real[home][at : at + 1, :]
                pivot_row = a[home][at : at + 1, :] * inverse
                turned_row = ia[home][at : at + 1, :] * inverse
                later = [
                    (d, real[home][at + d - c : at + d - c + 1, :] * inverse, imag[home][at + d - c : at + d - c + 1, :] * inverse)
                    for d in range(c + 1, PANEL)
                ]
                for g in range(home + (at == 7), groups):
                    fr, fi = real[g], imag[g]
                    if g == home:
                        fr, fi = jnp.where(row > at, fr, 0.0), jnp.where(row > at, fi, 0.0)
                    for d, x, y in later:
                        panel[2 * d][g] = panel[2 * d][g] - (fr * x + fi * y)
                        panel[2 * d + 1][g] = panel[2 * d + 1][g] - (fi * x - fr * y)
                    a[g] = a[g] - (fr * pivot_row + fi * turned_row)
                    ia[g] = ia[g] - (fr * turned_row - fi * pivot_row)
    lane, line = iota((users, LANES), 1), iota((users, LANES), 0)
    keep = (lane >= 2 * line) & (lane != 2 * line + 1) | (lane >= 2 * users)
    out = []
    for a in blocks:
        full = jnp.concatenate(a, axis=0)
        pivots = jnp.sum(jnp.where(lane == 2 * line, full, 0.0), axis=1, keepdims=True)
        scale = jnp.where(lane < 2 * users, constellation_norm, 1.0)
        out.append(jnp.where(keep, full * (lax.rsqrt(pivots) * scale), 0.0))
    return out


def kernel(
    dims, noise_any, gains_ref, samples_ref, branches_any, out_ref,
    noise_ref, branches_ref, held, raw, part, came, points, packed, taken,
    small_sem, load_sem, send_sem, recv_sem, usend_sem, urecv_sem,
):
    clusters, bands, users, symbols, share, mine_t, pieces = dims
    me, band = lax.axis_index("chain"), lax.axis_index("par")

    barrier = pltpu.get_barrier_semaphore()
    for k in range(1, clusters):
        pl.semaphore_signal(barrier, inc=1, device_id={"chain": lax.rem(me + k, clusters)}, device_id_type=MESH)
    for k in range(1, bands):
        pl.semaphore_signal(barrier, inc=1, device_id={"par": lax.rem(band + k, bands)}, device_id_type=MESH)

    order = list(range(1, clusters)) + [0]
    loads = {}
    for k in order:
        tones = pl.ds(lax.rem(me + k, clusters) * share, share)
        loads[k] = (
            pltpu.make_async_copy(
                gains_ref.at[0, tones], held.at[k, :, pl.ds(0, 2 * users)], load_sem.at[0, k]
            ),
            pltpu.make_async_copy(
                samples_ref.at[0, tones], held.at[k, :, pl.ds(2 * users, 2 * symbols)], load_sem.at[1, k]
            ),
        )
        for copy in loads[k]:
            copy.start()

    small = (
        pltpu.make_async_copy(noise_any, noise_ref, small_sem.at[0]),
        pltpu.make_async_copy(branches_any, branches_ref, small_sem.at[1]),
    )
    for copy in small:
        copy.start()
    raw[...] = jnp.zeros_like(raw)
    even = iota((users, LANES), 1) % 2 == 0
    sends = []
    for number, k in enumerate(order):
        for copy in loads[k]:
            copy.wait()
        for s in range(share):
            slot = (number * share + s) % raw.shape[0]
            both = held[k, s]
            raw[slot, :, : 2 * (users + symbols)] = lax.dot_general(
                both[: 2 * users], both, NT, preferred_element_type=jnp.float32
            )
            on_even = raw[slot, pl.ds(0, users, stride=2), :]
            on_odd = raw[slot, pl.ds(1, users, stride=2), :]
            part[k, s] = pair_swap(on_odd) + jnp.where(even, on_even, -on_even)
        if k:
            if number == 0:
                pl.semaphore_wait(barrier, clusters + bands - 2)
            copy = pltpu.make_async_remote_copy(
                src_ref=part.at[k], dst_ref=came.at[k], send_sem=send_sem.at[k], recv_sem=recv_sem.at[k],
                device_id={"chain": lax.rem(me + k, clusters)}, device_id_type=MESH,
            )
            copy.start()
            sends.append(copy)

    for copy in small:
        copy.wait()
    rows = pieces * mine_t
    source, target = iota((2 * LANES, 4 * LANES), 0), iota((2 * LANES, 4 * LANES), 1)
    place = target % (2 * LANES)
    user, quadrature, off = place // 2, place % 2, target // (2 * LANES)
    entry = jnp.where(source == user + LANES * ((quadrature + off) % 2), 1.0, 0.0)
    entry = jnp.where(off * quadrature == 1, -entry, entry).astype(jnp.bfloat16)
    marks = jnp.concatenate(
        [
            branches_ref[b, s, :, LANES * r : LANES * (r + 1)]
            for b in range(bands) for s in range(share) for r in range(pieces)
        ],
        axis=0,
    )
    pair = jnp.concatenate(
        [(2 * (marks & 7) - 7).astype(jnp.float32), (2 * (marks >> 3) - 7).astype(jnp.float32)], axis=1
    ).astype(jnp.bfloat16)
    woven = jnp.dot(pair, entry, preferred_element_type=jnp.float32).astype(jnp.bfloat16)
    for b in range(bands):
        for s in range(share):
            first = (b * share + s) * rows
            for h in range(2):
                for o in range(2):
                    points[b, s, pl.ds((2 * h + o) * rows, rows), :] = woven[
                        first : first + rows, LANES * (2 * o + h) : LANES * (2 * o + h + 1)
                    ]

    lane, line = iota((users, LANES), 1), iota((users, LANES), 0)
    noises = [
        jnp.sum(jnp.where(iota((1, bands), 1) == band, noise_ref[s : s + 1, :], 0.0), axis=1, keepdims=True)
        for s in range(share)
    ]
    totals = [part[0, s] for s in range(share)]
    for copy in sends:
        copy.wait_recv()
    for k in range(1, clusters):
        totals = [total + came[k, s] for s, total in enumerate(totals)]
    mats = [
        jnp.where(lane == 2 * line, total + noises[s], total) for s, total in enumerate(totals)
    ]
    factors = eliminate(mats, users)

    half, width, extra = users // 2, 2 * users, 2 * mine_t
    spot = iota((half, LANES), 1)
    for s, factor in enumerate(factors):
        top, bottom = factor[:half], factor[half:]
        turned = pltpu.roll(bottom, width, 1)
        for b in range(bands):
            upper = pltpu.roll(top, LANES - extra * b, 1) if b else top
            lower = pltpu.roll(bottom, (LANES + extra - extra * b) % LANES, 1) if b != 1 else bottom
            packed[b, s] = jnp.where(
                spot < width, top,
                jnp.where(spot >= width + users, turned, jnp.where(spot < width + extra, upper, lower)),
            )
    near = []
    inner = jnp.minimum(band, bands - 1 - band)
    outward = jnp.where(2 * band < bands - 1, 1, -1)
    for i in range(1, bands):
        both_sides = (i + 1) // 2 if i % 2 else -(i // 2)
        near.append(band + jnp.where(i <= 2 * inner, both_sides, outward * (i - inner)))
    usends = []
    for i in range(bands - 1, 0, -1):
        peer = near[i - 1]
        copy = pltpu.make_async_remote_copy(
            src_ref=packed.at[peer], dst_ref=taken.at[band], send_sem=usend_sem.at[i], recv_sem=urecv_sem.at[band],
            device_id={"par": peer}, device_id_type=MESH,
        )
        copy.start()
        usends.append(copy)

    r, c = iota((4 * rows, LANES), 0), iota((4 * rows, LANES), 1)
    is_off = (r // rows) % 2
    hit = ((c - width) % extra == 2 * (r % mine_t) + is_off) & (c >= width) & (c < width + 2 * extra)
    chosen = jnp.where(hit, (2 * is_off - 1).astype(jnp.float32), 0.0).astype(jnp.bfloat16)
    sr, sc = iota((width, LANES), 0), iota((width, LANES), 1)
    suffix = [
        jnp.where((sr // users + 2 * h == sc // users) & (sr % users >= sc % users), 1.0 / users, 0.0).astype(jnp.bfloat16)
        for h in range(2)
    ]
    for i in range(bands):
        b = band if i == 0 else near[i - 1]
        if i:
            pltpu.make_async_remote_copy(
                src_ref=packed.at[b], dst_ref=taken.at[b], send_sem=usend_sem.at[i], recv_sem=urecv_sem.at[b],
                device_id={"par": b}, device_id_type=MESH,
            ).wait_recv()
        box = taken if i else packed
        for s in range(share):
            folded = box[b, s]
            crossed = pltpu.roll(folded, width, 1)
            weights = jnp.concatenate(
                [
                    jnp.where(spot < width, folded, 0.0),
                    jnp.where((spot >= users) & (spot < width), crossed, 0.0),
                    jnp.where(spot >= width, crossed, 0.0),
                    jnp.where(spot >= width + users, folded, 0.0),
                ],
                axis=0,
            )
            own = [
                jnp.where((spot >= width) & (spot < width + extra), folded, 0.0),
                jnp.where((spot >= width + extra) & (spot < width + 2 * extra), folded, 0.0),
            ]
            high, low = split(jnp.concatenate([weights, jnp.concatenate(own + own, axis=0)], axis=1))
            p = jnp.concatenate([points[b, s], chosen], axis=1)
            rest = lax.dot_general(p, high, NT, preferred_element_type=jnp.float32) + lax.dot_general(
                p, low, NT, preferred_element_type=jnp.float32
            )
            result = None
            for h in range(2):
                on, off = rest[2 * h * rows : (2 * h + 1) * rows], rest[(2 * h + 1) * rows : (2 * h + 2) * rows]
                for term in split(on * on + off * off):
                    step = jnp.dot(term, suffix[h], preferred_element_type=jnp.float32)
                    result = step if result is None else result + step
            for r in range(pieces):
                out_ref[b, s, :, LANES * r : LANES * (r + 1)] = result[mine_t * r : mine_t * (r + 1)]
    for copy in sends + usends:
        copy.wait_send()


def local(propagation_gains, observed_samples, disturbance_variance, retained_branches):
    clusters, bands = lax.axis_size("chain"), lax.axis_size("par")
    _, tones, double_users, antennas = propagation_gains.shape
    users, symbols = double_users // 2, observed_samples.shape[2] // 2
    share, mine_t = tones // clusters, symbols // bands
    pieces = retained_branches.shape[-1] // LANES
    dims = (clusters, bands, users, symbols, share, mine_t, pieces)
    f32, bf16 = jnp.float32, jnp.bfloat16
    vmem, dma = pltpu.VMEM, pltpu.SemaphoreType.DMA
    payload = users // 2
    return pl.pallas_call(
        functools.partial(kernel, dims),
        out_shape=pltpu.VMEM(retained_branches.shape, f32),
        in_specs=[
            pl.BlockSpec(memory_space=pl.ANY),
            pl.BlockSpec(memory_space=pl.ANY),
            pl.BlockSpec(memory_space=pl.ANY),
            pl.BlockSpec(memory_space=pl.ANY),
        ],
        out_specs=pl.BlockSpec(memory_space=pltpu.VMEM),
        scratch_shapes=[
            vmem(disturbance_variance.shape[::-1], f32),
            vmem(retained_branches.shape, jnp.int32),
            vmem((clusters, share, 2 * (users + symbols), antennas), bf16),
            vmem((4, 2 * users, LANES), f32),
            vmem((clusters, share, users, LANES), f32),
            vmem((clusters, share, users, LANES), f32),
            vmem((bands, share, 4 * pieces * mine_t, LANES), bf16),
            vmem((bands, share, payload, LANES), f32),
            vmem((bands, share, payload, LANES), f32),
            dma((2,)), dma((2, clusters)), dma((clusters,)), dma((clusters,)), dma((bands,)), dma((bands,)),
        ],
        compiler_params=pltpu.CompilerParams(collective_id=0, has_side_effects=True),
        name="detect",
    )(*(
        pltpu.with_memory_space_constraint(x, pltpu.HBM)
        for x in (disturbance_variance.T, propagation_gains, observed_samples, retained_branches)
    ))


def solution(mesh):
    placed = (
        P("par", None, None, "chain"),
        P("par", None, None, "chain"),
        P(None, "chain"),
        P(None, "chain", "par", None),
    )
    return jax.shard_map(
        local, mesh=mesh, in_specs=placed, out_specs=P(None, "chain", "par", None), check_vma=False
    )
```

```python
import functools
import jax
import jax.numpy as jnp
from jax import lax
from jax.experimental import pallas as pl
from jax.experimental.pallas import tpu as pltpu
from jax.sharding import PartitionSpec as P

constellation_norm = 1.0 / 42.0**0.5
LANES = 128
PANEL = 4
MESH = pl.DeviceIdType.MESH
NT = (((1,), (1,)), ((), ()))


def iota(shape, dim):
    return lax.broadcasted_iota(jnp.int32, shape, dim)


def split(x):
    high = x.astype(jnp.bfloat16)
    return high, (x - high.astype(jnp.float32)).astype(jnp.bfloat16)


def pair_swap(x):
    even = iota(x.shape, 1) % 2 == 0
    return jnp.where(even, pltpu.roll(x, LANES - 1, 1), pltpu.roll(x, 1, 1))


def eliminate(mats, users):
    groups = users // 8
    blocks, turned = [], []
    for mat in mats:
        odd = iota((8, LANES), 1) % 2 == 1
        parts = [mat[8 * g : 8 * g + 8, :] for g in range(groups)]
        blocks.append(parts)
        turned.append([jnp.where(odd, pair_swap(p), -pair_swap(p)) for p in parts])
    row, lanes = iota((8, LANES), 0), iota((8, LANES), 1)
    for start in range(0, users, PANEL):
        home = start // 8
        panels = []
        for a in blocks:
            panel = []
            for j in range(start, start + PANEL):
                pivot = jnp.broadcast_to(a[home][j % 8 : j % 8 + 1, :], (8, LANES)) if start < users // 2 else None
                for part in range(2):
                    column = {}
                    for g in range(home, groups):
                        if start < users // 2 <= 8 * g:
                            found = jnp.where(lanes == 2 * (row + 8 * g) + part, pivot, 0.0)
                            found = jnp.sum(-found if part else found, axis=1, keepdims=True)
                        else:
                            found = a[g][:, 2 * j + part : 2 * j + part + 1]
                        column[g] = jnp.broadcast_to(found, (8, LANES))
                    panel.append(column)
            panels.append(panel)
        for j in range(start, min(start + PANEL, users - 1)):
            at, c = j % 8, j - start
            for a, ia, panel in zip(blocks, turned, panels):
                real, imag = panel[2 * c], panel[2 * c + 1]
                inverse = 1.0 / real[home][at : at + 1, :]
                pivot_row = a[home][at : at + 1, :] * inverse
                turned_row = ia[home][at : at + 1, :] * inverse
                later = [
                    (d, real[home][at + d - c : at + d - c + 1, :] * inverse, imag[home][at + d - c : at + d - c + 1, :] * inverse)
                    for d in range(c + 1, PANEL)
                ]
                for g in range(home + (at == 7), groups):
                    fr, fi = real[g], imag[g]
                    if g == home:
                        fr, fi = jnp.where(row > at, fr, 0.0), jnp.where(row > at, fi, 0.0)
                    for d, x, y in later:
                        panel[2 * d][g] = panel[2 * d][g] - (fr * x + fi * y)
                        panel[2 * d + 1][g] = panel[2 * d + 1][g] - (fi * x - fr * y)
                    a[g] = a[g] - (fr * pivot_row + fi * turned_row)
                    ia[g] = ia[g] - (fr * turned_row - fi * pivot_row)
    lane, line = iota((users, LANES), 1), iota((users, LANES), 0)
    keep = (lane >= 2 * line) & (lane != 2 * line + 1) | (lane >= 2 * users)
    out = []
    for a in blocks:
        full = jnp.concatenate(a, axis=0)
        pivots = jnp.sum(jnp.where(lane == 2 * line, full, 0.0), axis=1, keepdims=True)
        scale = jnp.where(lane < 2 * users, constellation_norm, 1.0)
        out.append(jnp.where(keep, full * (lax.rsqrt(pivots) * scale), 0.0))
    return out


def kernel(
    dims, noise_any, gains_ref, samples_ref, branches_any, out_ref,
    noise_ref, branches_ref, held, raw, part, came, points, packed, taken,
    small_sem, load_sem, send_sem, recv_sem, usend_sem, urecv_sem,
):
    clusters, bands, users, symbols, share, mine_t, pieces, compact = dims
    me, band = lax.axis_index("chain"), lax.axis_index("par")

    barrier = pltpu.get_barrier_semaphore()
    for k in range(1, clusters):
        pl.semaphore_signal(barrier, inc=1, device_id={"chain": lax.rem(me + k, clusters)}, device_id_type=MESH)
    for k in range(1, bands):
        pl.semaphore_signal(barrier, inc=1, device_id={"par": lax.rem(band + k, bands)}, device_id_type=MESH)

    order = list(range(clusters - 1, -1, -1))
    peers = {}
    for k in order:
        peers[k], bit = me - me, 1
        while bit < clusters:
            digit = lax.rem(me // bit, 2)
            peers[k] = peers[k] + bit * (1 - digit if (k // bit) % 2 else digit)
            bit *= 2
    loads = {}
    for k in order:
        tones = pl.ds(peers[k] * share, share)
        loads[k] = (
            pltpu.make_async_copy(
                gains_ref.at[0, tones], held.at[k, :, pl.ds(0, 2 * users)], load_sem.at[0, k]
            ),
            pltpu.make_async_copy(
                samples_ref.at[0, tones], held.at[k, :, pl.ds(2 * users, 2 * symbols)], load_sem.at[1, k]
            ),
        )
        for copy in loads[k]:
            copy.start()

    small = (
        pltpu.make_async_copy(noise_any, noise_ref, small_sem.at[0]),
        pltpu.make_async_copy(branches_any, branches_ref, small_sem.at[1]),
    )
    for copy in small:
        copy.start()
    raw[...] = jnp.zeros_like(raw)
    half, width = users // 2, 2 * users
    even, at = iota((users, LANES), 1) % 2 == 0, iota((half, LANES), 1)
    at8 = iota((8, LANES), 1) // users
    sends = []

    def fold(number, k, products):
        tiles = []
        for s, product in enumerate(products):
            slot = (number * share + s) % raw.shape[0]
            raw[slot, :, : width + 2 * symbols] = product
            on_even = raw[slot, pl.ds(0, users, stride=2), :]
            on_odd = raw[slot, pl.ds(1, users, stride=2), :]
            whole = pair_swap(on_odd) + jnp.where(even, on_even, -on_even)
            if not compact:
                part[k, s * users : (s + 1) * users] = whole
                continue
            lower = whole[half:]
            moved = pltpu.roll(lower, users, 1)
            part[k, s * half : (s + 1) * half] = jnp.where(at < 3 * users, whole[:half], moved)
            tiles.append((lower[:8], lower[8:], moved[:8]))
        if compact:
            (first, second, turned), (third, fourth, _) = tiles
            part[k, share * half :] = jnp.where(
                at8 == 0, pltpu.roll(third, LANES - users, 1),
                jnp.where(at8 == 1, second, jnp.where(at8 == 2, turned, pltpu.roll(fourth, 2 * users, 1))),
            )
        if k:
            if number == 0:
                pl.semaphore_wait(barrier, clusters + bands - 2)
            copy = pltpu.make_async_remote_copy(
                src_ref=part.at[k], dst_ref=came.at[k], send_sem=send_sem.at[k], recv_sem=recv_sem.at[k],
                device_id={"chain": peers[k]}, device_id_type=MESH,
            )
            copy.start()
            sends.append(copy)

    waiting = None
    for number, k in enumerate(order):
        for copy in loads[k]:
            copy.wait()
        products = []
        for s in range(share):
            both = held[k, s]
            products.append(lax.dot_general(both[:width], both, NT, preferred_element_type=jnp.float32))
        if waiting:
            fold(*waiting)
        waiting = (number, k, products)
    fold(*waiting)

    for copy in small:
        copy.wait()
    rows = pieces * mine_t
    source, target = iota((2 * LANES, 4 * LANES), 0), iota((2 * LANES, 4 * LANES), 1)
    place = target % (2 * LANES)
    user, quadrature, off = place // 2, place % 2, target // (2 * LANES)
    entry = jnp.where(source == user + LANES * ((quadrature + off) % 2), 1.0, 0.0)
    entry = jnp.where(off * quadrature == 1, -entry, entry).astype(jnp.bfloat16)
    marks = jnp.concatenate(
        [
            branches_ref[b, s, :, LANES * r : LANES * (r + 1)]
            for b in range(bands) for s in range(share) for r in range(pieces)
        ],
        axis=0,
    )
    pair = jnp.concatenate(
        [(2 * (marks & 7) - 7).astype(jnp.float32), (2 * (marks >> 3) - 7).astype(jnp.float32)], axis=1
    ).astype(jnp.bfloat16)
    woven = jnp.dot(pair, entry, preferred_element_type=jnp.float32).astype(jnp.bfloat16)
    for b in range(bands):
        for s in range(share):
            first = (b * share + s) * rows
            for h in range(2):
                for o in range(2):
                    points[b, s, pl.ds((2 * h + o) * rows, rows), :] = woven[
                        first : first + rows, LANES * (2 * o + h) : LANES * (2 * o + h + 1)
                    ]

    lane, line = iota((users, LANES), 1), iota((users, LANES), 0)
    noises = [
        jnp.sum(jnp.where(iota((1, bands), 1) == band, noise_ref[s : s + 1, :], 0.0), axis=1, keepdims=True)
        for s in range(share)
    ]
    for copy in sends:
        copy.wait_recv()
    total = part[0]
    for k in range(1, clusters):
        total = total + came[k]
    if compact:
        tile, mats = total[share * half :], []
        for s in range(share):
            upper = total[s * half : (s + 1) * half]
            back = pltpu.roll(upper, LANES - users, 1)
            corner = jnp.concatenate(
                [pltpu.roll(tile, LANES - users, 1), tile] if s == 0
                else [pltpu.roll(tile, users, 1), pltpu.roll(tile, 2 * users, 1)],
                axis=0,
            )
            lower = jnp.where((at >= users) & (at < width), corner, jnp.where((at >= width) & (at < 3 * users), back, 0.0))
            mats.append(jnp.concatenate([jnp.where(at < 3 * users, upper, 0.0), lower], axis=0))
    else:
        mats = [total[s * users : (s + 1) * users] for s in range(share)]
    mats = [jnp.where(lane == 2 * line, mat + noises[s], mat) for s, mat in enumerate(mats)]
    factors = eliminate(mats, users)

    extra, spot = 2 * mine_t, at
    for s, factor in enumerate(factors):
        top, bottom = factor[:half], factor[half:]
        turned = pltpu.roll(bottom, width, 1)
        for b in range(bands):
            upper = pltpu.roll(top, LANES - extra * b, 1) if b else top
            lower = pltpu.roll(bottom, (LANES + extra - extra * b) % LANES, 1) if b != 1 else bottom
            packed[b, s] = jnp.where(
                spot < width, top,
                jnp.where(spot >= width + users, turned, jnp.where(spot < width + extra, upper, lower)),
            )
    near = []
    inner = jnp.minimum(band, bands - 1 - band)
    outward = jnp.where(2 * band < bands - 1, 1, -1)
    for i in range(1, bands):
        both_sides = (i + 1) // 2 if i % 2 else -(i // 2)
        near.append(band + jnp.where(i <= 2 * inner, both_sides, outward * (i - inner)))
    usends = []
    for i in range(bands - 1, 0, -1):
        peer = near[i - 1]
        copy = pltpu.make_async_remote_copy(
            src_ref=packed.at[peer], dst_ref=taken.at[band], send_sem=usend_sem.at[i], recv_sem=urecv_sem.at[band],
            device_id={"par": peer}, device_id_type=MESH,
        )
        copy.start()
        usends.append(copy)

    r, c = iota((4 * rows, LANES), 0), iota((4 * rows, LANES), 1)
    is_off = (r // rows) % 2
    hit = ((c - width) % extra == 2 * (r % mine_t) + is_off) & (c >= width) & (c < width + 2 * extra)
    chosen = jnp.where(hit, (2 * is_off - 1).astype(jnp.float32), 0.0).astype(jnp.bfloat16)
    sr, sc = iota((width, LANES), 0), iota((width, LANES), 1)
    suffix = [
        jnp.where((sr // users + 2 * h == sc // users) & (sr % users >= sc % users), 1.0 / users, 0.0).astype(jnp.bfloat16)
        for h in range(2)
    ]
    for i in range(bands):
        b = band if i == 0 else near[i - 1]
        if i:
            pltpu.make_async_remote_copy(
                src_ref=packed.at[b], dst_ref=taken.at[b], send_sem=usend_sem.at[i], recv_sem=urecv_sem.at[b],
                device_id={"par": b}, device_id_type=MESH,
            ).wait_recv()
        box = taken if i else packed
        for s in range(share):
            folded = box[b, s]
            crossed = pltpu.roll(folded, width, 1)
            weights = jnp.concatenate(
                [
                    jnp.where(spot < width, folded, 0.0),
                    jnp.where((spot >= users) & (spot < width), crossed, 0.0),
                    jnp.where(spot >= width, crossed, 0.0),
                    jnp.where(spot >= width + users, folded, 0.0),
                ],
                axis=0,
            )
            own = [
                jnp.where((spot >= width) & (spot < width + extra), folded, 0.0),
                jnp.where((spot >= width + extra) & (spot < width + 2 * extra), folded, 0.0),
            ]
            high, low = split(jnp.concatenate([weights, jnp.concatenate(own + own, axis=0)], axis=1))
            p = jnp.concatenate([points[b, s], chosen], axis=1)
            rest = lax.dot_general(p, high, NT, preferred_element_type=jnp.float32) + lax.dot_general(
                p, low, NT, preferred_element_type=jnp.float32
            )
            result = None
            for h in range(2):
                on, off = rest[2 * h * rows : (2 * h + 1) * rows], rest[(2 * h + 1) * rows : (2 * h + 2) * rows]
                for term in split(on * on + off * off):
                    step = jnp.dot(term, suffix[h], preferred_element_type=jnp.float32)
                    result = step if result is None else result + step
            for r in range(pieces):
                out_ref[b, s, :, LANES * r : LANES * (r + 1)] = result[mine_t * r : mine_t * (r + 1)]
    for copy in sends + usends:
        copy.wait_send()


def local(propagation_gains, observed_samples, disturbance_variance, retained_branches):
    clusters, bands = lax.axis_size("chain"), lax.axis_size("par")
    _, tones, double_users, antennas = propagation_gains.shape
    users, symbols = double_users // 2, observed_samples.shape[2] // 2
    share, mine_t = tones // clusters, symbols // bands
    pieces = retained_branches.shape[-1] // LANES
    compact = share == 2 and users == 32 and 2 * symbols <= users
    lines = share * users // 2 + 8 if compact else share * users
    dims = (clusters, bands, users, symbols, share, mine_t, pieces, compact)
    f32, bf16 = jnp.float32, jnp.bfloat16
    vmem, dma = pltpu.VMEM, pltpu.SemaphoreType.DMA
    payload = users // 2
    return pl.pallas_call(
        functools.partial(kernel, dims),
        out_shape=pltpu.VMEM(retained_branches.shape, f32),
        in_specs=[
            pl.BlockSpec(memory_space=pl.ANY),
            pl.BlockSpec(memory_space=pl.ANY),
            pl.BlockSpec(memory_space=pl.ANY),
            pl.BlockSpec(memory_space=pl.ANY),
        ],
        out_specs=pl.BlockSpec(memory_space=pltpu.VMEM),
        scratch_shapes=[
            vmem(disturbance_variance.shape[::-1], f32),
            vmem(retained_branches.shape, jnp.int32),
            vmem((clusters, share, 2 * (users + symbols), antennas), bf16),
            vmem((4, 2 * users, LANES), f32),
            vmem((clusters, lines, LANES), f32),
            vmem((clusters, lines, LANES), f32),
            vmem((bands, share, 4 * pieces * mine_t, LANES), bf16),
            vmem((bands, share, payload, LANES), f32),
            vmem((bands, share, payload, LANES), f32),
            dma((2,)), dma((2, clusters)), dma((clusters,)), dma((clusters,)), dma((bands,)), dma((bands,)),
        ],
        compiler_params=pltpu.CompilerParams(collective_id=0, has_side_effects=True),
        name="detect",
    )(*(
        pltpu.with_memory_space_constraint(x, pltpu.HBM)
        for x in (disturbance_variance.T, propagation_gains, observed_samples, retained_branches)
    ))


def solution(mesh):
    placed = (
        P("par", None, None, "chain"),
        P("par", None, None, "chain"),
        P(None, "chain"),
        P(None, "chain", "par", None),
    )
    return jax.shard_map(
        local, mesh=mesh, in_specs=placed, out_specs=P(None, "chain", "par", None), check_vma=False
    )
```

```python
import functools
import jax
import jax.numpy as jnp
from jax import lax
from jax.experimental import pallas as pl
from jax.experimental.pallas import tpu as pltpu
from jax.sharding import PartitionSpec as P

constellation_norm = 1.0 / 42.0**0.5
LANES = 128
MESH = pl.DeviceIdType.MESH
NT = (((1,), (1,)), ((), ()))


def iota(shape, dim):
    return lax.broadcasted_iota(jnp.int32, shape, dim)


def panels(users):
    wide = users // 2
    return [(j, 4) for j in range(0, wide, 4)] + [(j, 8) for j in range(wide, users, 8)]


def split(x):
    high = x.astype(jnp.bfloat16)
    return high, (x - high.astype(jnp.float32)).astype(jnp.bfloat16)


def pair_swap(x):
    even = iota(x.shape, 1) % 2 == 0
    return jnp.where(even, pltpu.roll(x, LANES - 1, 1), pltpu.roll(x, 1, 1))


def eliminate(lines, users):
    groups, width = users // 8, 2 * users
    row, lanes = iota((8, LANES), 0), iota((8, LANES), 1)
    spot, second = lanes % width, lanes >= width
    a = list(lines)
    ia = [jnp.where(lanes % 2 == 1, pair_swap(p), -pair_swap(p)) for p in a[:groups]]
    by_row = [jnp.ones((8, LANES), jnp.float32) for _ in range(groups)]
    by_lane = jnp.ones((8, LANES), jnp.float32)

    def column(x, at):
        return jnp.where(second, x[:, width + at : width + at + 1], x[:, at : at + 1])

    for start, size in panels(users):
        home = start // 8
        panel = []
        for j in range(start, start + size):
            pivot = jnp.broadcast_to(a[home][j % 8 : j % 8 + 1, :], (8, LANES))
            for c in range(2):
                found = {}
                for g in range(home, len(a)):
                    if start < users // 2 <= 8 * g < users:
                        ones = [
                            jnp.sum(jnp.where(lanes == t * width + 2 * (row + 8 * g) + c, pivot, 0.0), axis=1, keepdims=True)
                            for t in range(2)
                        ]
                        found[g] = jnp.where(second, ones[1], ones[0])
                        if c:
                            found[g] = -found[g]
                    else:
                        found[g] = column(a[g], 2 * j + c)
                panel.append(found)
        for j in range(start, start + size):
            at, c = j % 8, j - start
            real, imag = panel[2 * c], panel[2 * c + 1]
            top = real[home][at : at + 1, :]
            root, inverse = lax.rsqrt(top), 1.0 / top
            by_row[home] = jnp.where(row == at, root, by_row[home])
            by_lane = jnp.where(spot // 2 == j, root, by_lane)
            beyond = spot[:1] > 2 * j + 1
            pivot_row = jnp.where(beyond, a[home][at : at + 1, :] * inverse, 0.0)
            turned_row = jnp.where(beyond, ia[home][at : at + 1, :] * inverse, 0.0)
            later = [
                (d, real[home][at + d - c : at + d - c + 1, :] * inverse, imag[home][at + d - c : at + d - c + 1, :] * inverse)
                for d in range(c + 1, size)
            ]
            for g in range(home, len(a)):
                if g == home and at == 7:
                    continue
                fr, fi = real[g], imag[g]
                if g == home:
                    fr, fi = jnp.where(row > at, fr, 0.0), jnp.where(row > at, fi, 0.0)
                for d, x, y in later:
                    panel[2 * d][g] = panel[2 * d][g] - (fr * x + fi * y)
                    panel[2 * d + 1][g] = panel[2 * d + 1][g] - (fi * x - fr * y)
                if j < users - 1:
                    a[g] = a[g] - (fr * pivot_row + fi * turned_row)
                    if g < groups:
                        ia[g] = ia[g] - (fr * turned_row - fi * pivot_row)
    upper = []
    for g in range(groups):
        diagonal = 2 * (row + 8 * g)
        keep = (spot >= diagonal) & (spot != diagonal + 1)
        upper.append(jnp.where(keep, a[g] * (by_row[g] * constellation_norm), 0.0))
    return upper, [x * by_lane for x in a[groups:]]


def kernel(
    dims, noise_any, gains_ref, samples_ref, branches_any, out_ref,
    noise_ref, branches_ref, held, raw, part, came, points, packed, taken,
    small_sem, load_sem, send_sem, recv_sem, usend_sem, urecv_sem,
):
    clusters, bands, users, symbols, share, mine_t, pieces = dims
    me, band = lax.axis_index("chain"), lax.axis_index("par")

    barrier = pltpu.get_barrier_semaphore()
    for k in range(1, clusters):
        pl.semaphore_signal(barrier, inc=1, device_id={"chain": lax.rem(me + k, clusters)}, device_id_type=MESH)
    for k in range(1, bands):
        pl.semaphore_signal(barrier, inc=1, device_id={"par": lax.rem(band + k, bands)}, device_id_type=MESH)

    order = list(range(clusters - 1, -1, -1))
    peers = {}
    for k in order:
        peers[k], bit = me - me, 1
        while bit < clusters:
            digit = lax.rem(me // bit, 2)
            peers[k] = peers[k] + bit * (1 - digit if (k // bit) % 2 else digit)
            bit *= 2
    loads = {}
    for k in order:
        tones = pl.ds(peers[k] * share, share)
        loads[k] = (
            pltpu.make_async_copy(
                gains_ref.at[0, tones], held.at[k, :, pl.ds(0, 2 * users)], load_sem.at[0, k]
            ),
            pltpu.make_async_copy(
                samples_ref.at[0, tones], held.at[k, :, pl.ds(2 * users, 2 * symbols)], load_sem.at[1, k]
            ),
        )
        for copy in loads[k]:
            copy.start()

    small = (
        pltpu.make_async_copy(noise_any, noise_ref, small_sem.at[0]),
        pltpu.make_async_copy(branches_any, branches_ref, small_sem.at[1]),
    )
    for copy in small:
        copy.start()
    half, quarter, width, depth = users // 2, users // 4, 2 * users, 2 * (users + symbols)
    sends = []

    def fold(number, k, product):
        slot = number % raw.shape[0]
        raw[slot] = jnp.where(iota((depth, LANES), 1) < width, product[:depth], product[depth:])
        on_even = raw[slot, pl.ds(0, depth // 2, stride=2), :]
        on_odd = raw[slot, pl.ds(1, depth // 2, stride=2), :]
        even = iota((depth // 2, LANES), 1) % 2 == 0
        whole = pair_swap(on_odd) + jnp.where(even, on_even, -on_even)
        part[k, :half] = whole[:half]
        part[k, half : half + quarter] = jnp.where(
            iota((quarter, LANES), 1) % width >= users,
            whole[half + quarter : users],
            pltpu.roll(whole[half : half + quarter], LANES - users, 1),
        )
        part[k, half + quarter :] = whole[users:]
        if k:
            if number == 0:
                pl.semaphore_wait(barrier, clusters + bands - 2)
            copy = pltpu.make_async_remote_copy(
                src_ref=part.at[k], dst_ref=came.at[k], send_sem=send_sem.at[k], recv_sem=recv_sem.at[k],
                device_id={"chain": peers[k]}, device_id_type=MESH,
            )
            copy.start()
            sends.append(copy)

    waiting = None
    for number, k in enumerate(order):
        for copy in loads[k]:
            copy.wait()
        fixed = jnp.concatenate([held[k, s, :width] for s in range(share)], axis=0)
        streamed = jnp.concatenate([held[k, s] for s in range(share)], axis=0)
        product = lax.dot_general(streamed, fixed, NT, preferred_element_type=jnp.float32)
        if waiting:
            fold(*waiting)
        waiting = (number, k, product)
    fold(*waiting)

    for copy in small:
        copy.wait()
    rows = pieces * mine_t
    source, target = iota((2 * LANES, 4 * LANES), 0), iota((2 * LANES, 4 * LANES), 1)
    place = target % (2 * LANES)
    user, quadrature, off = place // 2, place % 2, target // (2 * LANES)
    entry = jnp.where(source == user + LANES * ((quadrature + off) % 2), 1.0, 0.0)
    entry = jnp.where(off * quadrature == 1, -entry, entry).astype(jnp.bfloat16)
    marks = jnp.concatenate(
        [
            branches_ref[b, s, :, LANES * r : LANES * (r + 1)]
            for b in range(bands) for s in range(share) for r in range(pieces)
        ],
        axis=0,
    )
    pair = jnp.concatenate(
        [(2 * (marks & 7) - 7).astype(jnp.float32), (2 * (marks >> 3) - 7).astype(jnp.float32)], axis=1
    ).astype(jnp.bfloat16)
    woven = jnp.dot(pair, entry, preferred_element_type=jnp.float32).astype(jnp.bfloat16)
    for b in range(bands):
        for s in range(share):
            first = (b * share + s) * rows
            for h in range(2):
                for o in range(2):
                    points[b, s, pl.ds((2 * h + o) * rows, rows), :] = woven[
                        first : first + rows, LANES * (2 * o + h) : LANES * (2 * o + h + 1)
                    ]

    noises = [
        jnp.sum(jnp.where(iota((1, bands), 1) == band, noise_ref[s : s + 1, :], 0.0), axis=1, keepdims=True)
        for s in range(share)
    ]
    row, lanes = iota((8, LANES), 0), iota((8, LANES), 1)
    noise = jnp.where(lanes >= width, noises[1], noises[0])
    for copy in sends:
        copy.wait_recv()
    total = part[0]
    for k in range(1, clusters):
        total = total + came[k]
    corner = total[half : half + quarter]
    inside = iota((quarter, LANES), 1) % width >= users
    lower = [jnp.where(inside, x, 0.0) for x in (pltpu.roll(corner, users, 1), corner)]
    mats = jnp.concatenate([total[:half]] + lower + [total[half + quarter :]], axis=0)
    lines = [mats[8 * g : 8 * g + 8] for g in range((users + symbols) // 8)]
    for g in range(users // 8):
        lines[g] = jnp.where(lanes % width == 2 * (row + 8 * g), lines[g] + noise, lines[g])
    upper, rotated = eliminate(lines, users)
    upper, rotated = jnp.concatenate(upper, axis=0), jnp.concatenate(rotated, axis=0)
    corner = jnp.where(inside, upper[half + quarter :], pltpu.roll(upper[half : half + quarter], LANES - users, 1))
    for b in range(bands):
        packed[b, :half] = upper[:half]
        packed[b, half : half + quarter] = corner
        packed[b, half + quarter :] = rotated[mine_t * b : mine_t * (b + 1)]
    near = []
    inner = jnp.minimum(band, bands - 1 - band)
    outward = jnp.where(2 * band < bands - 1, 1, -1)
    for i in range(1, bands):
        both_sides = (i + 1) // 2 if i % 2 else -(i // 2)
        near.append(band + jnp.where(i <= 2 * inner, both_sides, outward * (i - inner)))
    usends = []
    for i in range(bands - 1, 0, -1):
        peer = near[i - 1]
        copy = pltpu.make_async_remote_copy(
            src_ref=packed.at[peer], dst_ref=taken.at[band], send_sem=usend_sem.at[i], recv_sem=urecv_sem.at[band],
            device_id={"par": peer}, device_id_type=MESH,
        )
        copy.start()
        usends.append(copy)

    r, c = iota((width, LANES), 0), iota((width, LANES), 1)
    minus = jnp.where(c % width // 2 == r % users, -1.0, 0.0).astype(jnp.bfloat16)
    sr, sc = iota((width, LANES), 0), iota((width, LANES), 1)
    suffix = [
        jnp.where((sr // users + 2 * h == sc // users) & (sr % users >= sc % users), 1.0 / users, 0.0).astype(jnp.bfloat16)
        for h in range(2)
    ]
    for i in range(bands):
        b = band if i == 0 else near[i - 1]
        if i:
            pltpu.make_async_remote_copy(
                src_ref=packed.at[b], dst_ref=taken.at[b], send_sem=usend_sem.at[i], recv_sem=urecv_sem.at[b],
                device_id={"par": b}, device_id_type=MESH,
            ).wait_recv()
        box = taken if i else packed
        top, corner = box[b, :half], box[b, half : half + quarter]
        straight = [(top, corner, pltpu.roll(corner, users, 1))]
        straight.append((pltpu.roll(top, width, 1), pltpu.roll(corner, width, 1), pltpu.roll(corner, 3 * users, 1)))
        z = box[b, half + quarter :]
        low = pltpu.roll(z, width, 1)
        low = low - low.astype(jnp.bfloat16).astype(jnp.float32)
        side, edge = iota(top.shape, 1) // width, iota(corner.shape, 1) // users
        for s in range(share):
            weights = []
            for e in range(2):
                above, fourth, third = straight[(s + e) % 2]
                weights += [
                    jnp.where(side == e, above, 0.0),
                    jnp.where(edge == 2 * e + 1, third, 0.0),
                    jnp.where(edge == 2 * e + 1, fourth, 0.0),
                ]
            high, rest_of = split(jnp.concatenate(weights, axis=0))
            zl = iota(z.shape, 1)
            both = jnp.where(zl // width == s, z, low)
            both = jnp.concatenate(
                [jnp.concatenate([jnp.where(zl % 2 == o, both, 0.0)] * pieces, axis=0) for o in range(2)] * 2, axis=0
            ).astype(jnp.bfloat16)
            p = points[b, s]
            rest = lax.dot_general(
                jnp.concatenate([p, both], axis=1), jnp.concatenate([high, minus], axis=1), NT,
                preferred_element_type=jnp.float32,
            ) + lax.dot_general(p, rest_of, NT, preferred_element_type=jnp.float32)
            result = None
            for h in range(2):
                on, off = rest[2 * h * rows : (2 * h + 1) * rows], rest[(2 * h + 1) * rows : (2 * h + 2) * rows]
                for term in split(on * on + off * off):
                    step = jnp.dot(term, suffix[h], preferred_element_type=jnp.float32)
                    result = step if result is None else result + step
            for r in range(pieces):
                out_ref[b, s, :, LANES * r : LANES * (r + 1)] = result[mine_t * r : mine_t * (r + 1)]
    for copy in sends + usends:
        copy.wait_send()


def local(propagation_gains, observed_samples, disturbance_variance, retained_branches):
    clusters, bands = lax.axis_size("chain"), lax.axis_size("par")
    _, tones, double_users, antennas = propagation_gains.shape
    users, symbols = double_users // 2, observed_samples.shape[2] // 2
    share, mine_t = tones // clusters, symbols // bands
    pieces = retained_branches.shape[-1] // LANES
    assert share == 2 and 4 * users == LANES
    dims = (clusters, bands, users, symbols, share, mine_t, pieces)
    lines = 3 * users // 4
    f32, bf16 = jnp.float32, jnp.bfloat16
    vmem, dma = pltpu.VMEM, pltpu.SemaphoreType.DMA
    return pl.pallas_call(
        functools.partial(kernel, dims),
        out_shape=pltpu.VMEM(retained_branches.shape, f32),
        in_specs=[
            pl.BlockSpec(memory_space=pl.ANY),
            pl.BlockSpec(memory_space=pl.ANY),
            pl.BlockSpec(memory_space=pl.ANY),
            pl.BlockSpec(memory_space=pl.ANY),
        ],
        out_specs=pl.BlockSpec(memory_space=pltpu.VMEM),
        scratch_shapes=[
            vmem(disturbance_variance.shape[::-1], f32),
            vmem(retained_branches.shape, jnp.int32),
            vmem((clusters, share, 2 * (users + symbols), antennas), bf16),
            vmem((2, 2 * (users + symbols), LANES), f32),
            vmem((clusters, lines + symbols, LANES), f32),
            vmem((clusters, lines + symbols, LANES), f32),
            vmem((bands, share, 4 * pieces * mine_t, LANES), bf16),
            vmem((bands, lines + mine_t, LANES), f32),
            vmem((bands, lines + mine_t, LANES), f32),
            dma((2,)), dma((2, clusters)), dma((clusters,)), dma((clusters,)), dma((bands,)), dma((bands,)),
        ],
        compiler_params=pltpu.CompilerParams(collective_id=0, has_side_effects=True),
        name="detect",
    )(*(
        pltpu.with_memory_space_constraint(x, pltpu.HBM)
        for x in (disturbance_variance.T, propagation_gains, observed_samples, retained_branches)
    ))


def solution(mesh):
    placed = (
        P("par", None, None, "chain"),
        P("par", None, None, "chain"),
        P(None, "chain"),
        P(None, "chain", "par", None),
    )
    return jax.shard_map(
        local, mesh=mesh, in_specs=placed, out_specs=P(None, "chain", "par", None), check_vma=False
    )
```

```python
import functools
import jax
import jax.numpy as jnp
from jax import lax
from jax.experimental import pallas as pl
from jax.experimental.pallas import tpu as pltpu
from jax.sharding import PartitionSpec as P

constellation_norm = 1.0 / 42.0**0.5
LANES = 128
MESH = pl.DeviceIdType.MESH
NT = (((1,), (1,)), ((), ()))


def iota(shape, dim):
    return lax.broadcasted_iota(jnp.int32, shape, dim)


def panels(users):
    wide = users // 2
    return [(j, 4) for j in range(0, wide, 4)] + [(j, 8) for j in range(wide, users, 8)]


def split(x):
    high = x.astype(jnp.bfloat16)
    return high, (x - high.astype(jnp.float32)).astype(jnp.bfloat16)


def pair_swap(x):
    even = iota(x.shape, 1) % 2 == 0
    return jnp.where(even, pltpu.roll(x, LANES - 1, 1), pltpu.roll(x, 1, 1))


def eliminate(a, q, users):
    groups, width = users // 8, 2 * users
    row, lanes = iota((8, LANES), 0), iota((8, LANES), 1)
    tone = jnp.where(lanes >= width, width, 0)
    ia, iq = [[jnp.where(lanes % 2 == 1, pair_swap(p), -pair_swap(p)) for p in x] for x in (a, q)]
    by_row = [jnp.ones((8, LANES), jnp.float32) for _ in range(groups)]
    for start, size in panels(users):
        home = start // 8
        panel = []
        for j in range(start, start + size):
            pivot = jnp.broadcast_to(a[home][j % 8 : j % 8 + 1, :], (8, LANES))
            for c in range(2):
                found = {}
                for g in range(home, groups):
                    if start < users // 2 <= 8 * g:
                        ones = [
                            jnp.sum(jnp.where(lanes == t * width + 2 * (row + 8 * g) + c, pivot, 0.0), axis=1, keepdims=True)
                            for t in range(2)
                        ]
                        found[g] = jnp.where(lanes >= width, ones[1], ones[0])
                        if c:
                            found[g] = -found[g]
                    else:
                        found[g] = jnp.take_along_axis(a[g], tone + (2 * j + c), axis=1, mode="promise_in_bounds")
                panel.append(found)
        for j in range(start, start + size):
            at, c = j % 8, j - start
            real, imag = panel[2 * c], panel[2 * c + 1]
            top = real[home][at : at + 1, :]
            by_row[home] = jnp.where(row == at, lax.rsqrt(top), by_row[home])
            if j == users - 1:
                break
            inverse = 1.0 / top
            pivots = [(x, ix, x[home][at : at + 1, :] * inverse, ix[home][at : at + 1, :] * inverse) for x, ix in ((a, ia), (q, iq))]
            later = [
                (d, real[home][at + d - c : at + d - c + 1, :] * inverse, imag[home][at + d - c : at + d - c + 1, :] * inverse)
                for d in range(c + 1, size)
            ]
            for g in range(home + (at == 7), groups):
                fr, fi = real[g], imag[g]
                if g == home:
                    fr, fi = jnp.where(row > at, fr, 0.0), jnp.where(row > at, fi, 0.0)
                for d, x, y in later:
                    panel[2 * d][g] = panel[2 * d][g] - (fr * x + fi * y)
                    panel[2 * d + 1][g] = panel[2 * d + 1][g] - (fi * x - fr * y)
                for x, ix, pivot_row, turned_row in pivots:
                    x[g] = x[g] - (fr * pivot_row + fi * turned_row)
                    ix[g] = ix[g] - (fr * turned_row - fi * pivot_row)
    upper = []
    for g in range(groups):
        diagonal = 2 * (row + 8 * g)
        keep = (lanes % width >= diagonal) & (lanes % width != diagonal + 1)
        upper.append(jnp.where(keep, a[g] * (by_row[g] * constellation_norm), 0.0))
    return upper, [x * scale for x, scale in zip(q, by_row)]


def kernel(
    dims, noise_any, gains_ref, samples_ref, branches_any, out_ref,
    noise_ref, branches_ref, held, raw, part, came, points, packed, taken,
    small_sem, load_sem, send_sem, recv_sem, usend_sem, urecv_sem,
):
    clusters, bands, users, symbols, share, mine_t, pieces = dims
    me, band = lax.axis_index("chain"), lax.axis_index("par")

    barrier = pltpu.get_barrier_semaphore()
    for k in range(1, clusters):
        pl.semaphore_signal(barrier, inc=1, device_id={"chain": lax.rem(me + k, clusters)}, device_id_type=MESH)
    for k in range(1, bands):
        pl.semaphore_signal(barrier, inc=1, device_id={"par": lax.rem(band + k, bands)}, device_id_type=MESH)

    order = list(range(clusters - 1, -1, -1))
    peers = {}
    for k in order:
        peers[k], bit = me - me, 1
        while bit < clusters:
            digit = lax.rem(me // bit, 2)
            peers[k] = peers[k] + bit * (1 - digit if (k // bit) % 2 else digit)
            bit *= 2
    loads = {}
    for k in order:
        tones = pl.ds(peers[k] * share, share)
        loads[k] = (
            pltpu.make_async_copy(
                gains_ref.at[0, tones], held.at[k, :, pl.ds(0, 2 * users)], load_sem.at[0, k]
            ),
            pltpu.make_async_copy(
                samples_ref.at[0, tones], held.at[k, :, pl.ds(2 * users, 2 * symbols)], load_sem.at[1, k]
            ),
        )
        for copy in loads[k]:
            copy.start()

    small = (
        pltpu.make_async_copy(noise_any, noise_ref, small_sem.at[0]),
        pltpu.make_async_copy(branches_any, branches_ref, small_sem.at[1]),
    )
    for copy in small:
        copy.start()
    half, quarter, width = users // 2, users // 4, 2 * users
    tail = share * half + quarter
    compact = 2 * symbols <= users
    at, edge8 = iota((half, LANES), 1), iota((quarter, LANES), 1) // users
    even = iota((users, LANES), 1) % 2 == 0
    sends = []

    def fold(number, k, products):
        lower = []
        for s, product in enumerate(products):
            slot = (number * share + s) % raw.shape[0]
            raw[slot, :, : width + 2 * symbols] = product
            on_even = raw[slot, pl.ds(0, users, stride=2), :]
            on_odd = raw[slot, pl.ds(1, users, stride=2), :]
            whole = pair_swap(on_odd) + jnp.where(even, on_even, -on_even)
            lower.append(whole[half:])
            upper = whole[:half]
            if compact:
                upper = jnp.where(at < 3 * users, upper, pltpu.roll(whole[half:], users, 1))
            part[k, s * half : (s + 1) * half] = upper
        part[k, share * half : tail] = jnp.where(
            edge8 == 0, pltpu.roll(lower[1][:quarter], 3 * users, 1),
            jnp.where(
                edge8 == 1, lower[0][quarter:],
                jnp.where(edge8 == 2, pltpu.roll(lower[0][:quarter], users, 1), pltpu.roll(lower[1][quarter:], width, 1)),
            ),
        )
        if not compact:
            part[k, tail:] = jnp.where(at < width, pltpu.roll(lower[0], width, 1), lower[1])
        if k:
            if number == 0:
                pl.semaphore_wait(barrier, clusters + bands - 2)
            copy = pltpu.make_async_remote_copy(
                src_ref=part.at[k], dst_ref=came.at[k], send_sem=send_sem.at[k], recv_sem=recv_sem.at[k],
                device_id={"chain": peers[k]}, device_id_type=MESH,
            )
            copy.start()
            sends.append(copy)

    raw[...] = jnp.zeros_like(raw)
    waiting = []
    numbered = list(enumerate(order))
    for lot in [numbered[:1]] + [numbered[i : i + 2] for i in range(1, clusters, 2)]:
        fresh = []
        for number, k in lot:
            for copy in loads[k]:
                copy.wait()
        for number, k in lot:
            products = []
            for s in range(share):
                both = held[k, s]
                products.append(lax.dot_general(both[:width], both, NT, preferred_element_type=jnp.float32))
            fresh.append((number, k, products))
        for chunk in waiting:
            fold(*chunk)
        waiting = fresh
    for chunk in waiting:
        fold(*chunk)

    for copy in small:
        copy.wait()
    rows = pieces * mine_t
    source, target = iota((2 * LANES, 4 * LANES), 0), iota((2 * LANES, 4 * LANES), 1)
    place = target % (2 * LANES)
    user, quadrature, off = place // 2, place % 2, target // (2 * LANES)
    entry = jnp.where(source == user + LANES * ((quadrature + off) % 2), 1.0, 0.0)
    entry = jnp.where(off * quadrature == 1, -entry, entry).astype(jnp.bfloat16)
    marks = jnp.concatenate(
        [
            branches_ref[b, s, :, LANES * r : LANES * (r + 1)]
            for b in range(bands) for s in range(share) for r in range(pieces)
        ],
        axis=0,
    )
    pair = jnp.concatenate(
        [(2 * (marks & 7) - 7).astype(jnp.float32), (2 * (marks >> 3) - 7).astype(jnp.float32)], axis=1
    ).astype(jnp.bfloat16)
    woven = jnp.dot(pair, entry, preferred_element_type=jnp.float32).astype(jnp.bfloat16)
    for b in range(bands):
        for s in range(share):
            first = (b * share + s) * rows
            for h in range(2):
                for o in range(2):
                    points[b, s, pl.ds((2 * h + o) * rows, rows), :] = woven[
                        first : first + rows, LANES * (2 * o + h) : LANES * (2 * o + h + 1)
                    ]

    noises = [
        jnp.sum(jnp.where(iota((1, bands), 1) == band, noise_ref[s : s + 1, :], 0.0), axis=1, keepdims=True)
        for s in range(share)
    ]
    row, lanes, extra = iota((8, LANES), 0), iota((8, LANES), 1), 2 * mine_t
    noise = jnp.where(lanes >= width, noises[1], noises[0])
    for copy in sends:
        copy.wait_recv()
    total = part[0]
    for k in range(1, clusters):
        total = total + came[k]
    tile, ups = total[share * half : tail], [total[s * half : (s + 1) * half] for s in range(share)]
    inside = iota((quarter, LANES), 1) % width >= users
    above = jnp.where(at < width, ups[0], pltpu.roll(ups[1], width, 1))
    below = [jnp.where(inside, x, 0.0) for x in (pltpu.roll(tile, 3 * users, 1), tile)]
    seen = [jnp.where(at < width, pltpu.roll(ups[0], width, 1), ups[1])]
    if compact:
        seen.append(jnp.where(at < width, pltpu.roll(ups[0], users, 1), pltpu.roll(ups[1], 3 * users, 1)))
    else:
        seen.append(total[tail:])
    seen = [jnp.where(at % width < 2 * symbols, x, 0.0) for x in seen]
    lines = [above[:8], above[8:]] + below
    for g in range(users // 8):
        lines[g] = jnp.where(lanes % width == 2 * (row + 8 * g), lines[g] + noise, lines[g])
    upper, rotated = eliminate(lines, [x[8 * i : 8 * i + 8] for x in seen for i in range(half // 8)], users)
    corner = jnp.where(inside, upper[3], pltpu.roll(upper[2], 3 * users, 1))
    for b in range(bands):
        z = jnp.zeros_like(corner)
        for g in range(users // 8):
            shift = extra * (g - b) % LANES
            z = jnp.where(lanes % width // extra == g, pltpu.roll(rotated[g], shift, 1) if shift else rotated[g], z)
        packed[b, :8] = upper[0]
        packed[b, 8:half] = upper[1]
        packed[b, half : half + quarter] = corner
        packed[b, half + quarter :] = z
    near = []
    inner = jnp.minimum(band, bands - 1 - band)
    outward = jnp.where(2 * band < bands - 1, 1, -1)
    for i in range(1, bands):
        both_sides = (i + 1) // 2 if i % 2 else -(i // 2)
        near.append(band + jnp.where(i <= 2 * inner, both_sides, outward * (i - inner)))
    usends = []
    for i in range(bands - 1, 0, -1):
        peer = near[i - 1]
        copy = pltpu.make_async_remote_copy(
            src_ref=packed.at[peer], dst_ref=taken.at[band], send_sem=usend_sem.at[i], recv_sem=urecv_sem.at[band],
            device_id={"par": peer}, device_id_type=MESH,
        )
        copy.start()
        usends.append(copy)

    r, c = iota((4 * rows, LANES), 0), iota((4 * rows, LANES), 1)
    is_off = (r // rows) % 2
    chosen = jnp.where(c % extra == 2 * (r % mine_t) + is_off, (2 * is_off - 1).astype(jnp.float32), 0.0).astype(jnp.bfloat16)
    sr, sc = iota((width, LANES), 0), iota((width, LANES), 1)
    suffix = [
        jnp.where((sr // users + 2 * h == sc // users) & (sr % users >= sc % users), 1.0 / users, 0.0).astype(jnp.bfloat16)
        for h in range(2)
    ]
    for i in range(bands):
        b = band if i == 0 else near[i - 1]
        if i:
            pltpu.make_async_remote_copy(
                src_ref=packed.at[b], dst_ref=taken.at[b], send_sem=usend_sem.at[i], recv_sem=urecv_sem.at[b],
                device_id={"par": b}, device_id_type=MESH,
            ).wait_recv()
        box = taken if i else packed
        top, corner = box[b, :half], box[b, half : half + quarter]
        straight = [(top, corner, pltpu.roll(corner, users, 1))]
        straight.append((pltpu.roll(top, width, 1), pltpu.roll(corner, width, 1), pltpu.roll(corner, 3 * users, 1)))
        z = box[b, half + quarter :]
        side, edge = iota(top.shape, 1) // width, iota(corner.shape, 1) // users
        for s in range(share):
            weights = []
            for e in range(2):
                above, fourth, third = straight[(s + e) % 2]
                weights += [
                    jnp.where(side == e, above, 0.0),
                    jnp.where(edge == 2 * e + 1, third, 0.0),
                    jnp.where(edge == 2 * e + 1, fourth, 0.0),
                ]
            own = [jnp.where(lanes // extra == width * s // extra + g, z, 0.0) for g in range(users // 8)]
            high, low = split(
                jnp.concatenate([jnp.concatenate(weights, axis=0), jnp.concatenate(own + own, axis=0)], axis=1)
            )
            p = jnp.concatenate([points[b, s], chosen], axis=1)
            rest = lax.dot_general(p, high, NT, preferred_element_type=jnp.float32) + lax.dot_general(
                p, low, NT, preferred_element_type=jnp.float32
            )
            result = None
            for h in range(2):
                on, off = rest[2 * h * rows : (2 * h + 1) * rows], rest[(2 * h + 1) * rows : (2 * h + 2) * rows]
                for term in split(on * on + off * off):
                    step = jnp.dot(term, suffix[h], preferred_element_type=jnp.float32)
                    result = step if result is None else result + step
            for r in range(pieces):
                out_ref[b, s, :, LANES * r : LANES * (r + 1)] = result[mine_t * r : mine_t * (r + 1)]
    for copy in sends + usends:
        copy.wait_send()


def local(propagation_gains, observed_samples, disturbance_variance, retained_branches):
    clusters, bands = lax.axis_size("chain"), lax.axis_size("par")
    _, tones, double_users, antennas = propagation_gains.shape
    users, symbols = double_users // 2, observed_samples.shape[2] // 2
    share, mine_t = tones // clusters, symbols // bands
    pieces = retained_branches.shape[-1] // LANES
    assert share == 2 and 4 * users == LANES and 4 * mine_t <= users // 2
    dims = (clusters, bands, users, symbols, share, mine_t, pieces)
    lines = share * users // 2 + users // 4 + (0 if 2 * symbols <= users else users // 2)
    f32, bf16 = jnp.float32, jnp.bfloat16
    vmem, dma = pltpu.VMEM, pltpu.SemaphoreType.DMA
    return pl.pallas_call(
        functools.partial(kernel, dims),
        out_shape=pltpu.VMEM(retained_branches.shape, f32),
        in_specs=[
            pl.BlockSpec(memory_space=pl.ANY),
            pl.BlockSpec(memory_space=pl.ANY),
            pl.BlockSpec(memory_space=pl.ANY),
            pl.BlockSpec(memory_space=pl.ANY),
        ],
        out_specs=pl.BlockSpec(memory_space=pltpu.VMEM),
        scratch_shapes=[
            vmem(disturbance_variance.shape[::-1], f32),
            vmem(retained_branches.shape, jnp.int32),
            vmem((clusters, share, 2 * (users + symbols), antennas), bf16),
            vmem((4, 2 * users, LANES), f32),
            vmem((clusters, lines, LANES), f32),
            vmem((clusters, lines, LANES), f32),
            vmem((bands, share, 4 * pieces * mine_t, LANES), bf16),
            vmem((bands, users, LANES), f32),
            vmem((bands, users, LANES), f32),
            dma((2,)), dma((2, clusters)), dma((clusters,)), dma((clusters,)), dma((bands,)), dma((bands,)),
        ],
        compiler_params=pltpu.CompilerParams(collective_id=0, has_side_effects=True),
        name="detect",
    )(*(
        pltpu.with_memory_space_constraint(x, pltpu.HBM)
        for x in (disturbance_variance.T, propagation_gains, observed_samples, retained_branches)
    ))


def solution(mesh):
    placed = (
        P("par", None, None, "chain"),
        P("par", None, None, "chain"),
        P(None, "chain"),
        P(None, "chain", "par", None),
    )
    return jax.shard_map(
        local, mesh=mesh, in_specs=placed, out_specs=P(None, "chain", "par", None), check_vma=False
    )
```

```python
import functools
import jax
import jax.numpy as jnp
from jax import lax
from jax.experimental import pallas as pl
from jax.experimental.pallas import tpu as pltpu
from jax.sharding import PartitionSpec as P

constellation_norm = 1.0 / 42.0**0.5
LANES = 128
MESH = pl.DeviceIdType.MESH
NT = (((1,), (1,)), ((), ()))


def iota(shape, dim):
    return lax.broadcasted_iota(jnp.int32, shape, dim)


def panels(users):
    wide = users // 2
    return [(j, 4) for j in range(0, wide, 4)] + [(j, 8) for j in range(wide, users, 8)]


def split(x):
    high = x.astype(jnp.bfloat16)
    return high, (x - high.astype(jnp.float32)).astype(jnp.bfloat16)


def pair_swap(x):
    even = iota(x.shape, 1) % 2 == 0
    return jnp.where(even, pltpu.roll(x, LANES - 1, 1), pltpu.roll(x, 1, 1))


def eliminate(a, q, users):
    groups, width = users // 8, 2 * users
    row, lanes = iota((8, LANES), 0), iota((8, LANES), 1)
    tone = jnp.where(lanes >= width, width, 0)
    ia, iq = [[jnp.where(lanes % 2 == 1, pair_swap(p), -pair_swap(p)) for p in x] for x in (a, q)]
    by_row = [jnp.ones((8, LANES), jnp.float32) for _ in range(groups)]
    for start, size in panels(users):
        home = start // 8
        panel = []
        for j in range(start, start + size):
            pivot = jnp.broadcast_to(a[home][j % 8 : j % 8 + 1, :], (8, LANES))
            for c in range(2):
                found = {}
                for g in range(home, groups):
                    if start < users // 2 <= 8 * g:
                        ones = [
                            jnp.sum(jnp.where(lanes == t * width + 2 * (row + 8 * g) + c, pivot, 0.0), axis=1, keepdims=True)
                            for t in range(2)
                        ]
                        found[g] = jnp.where(lanes >= width, ones[1], ones[0])
                        if c:
                            found[g] = -found[g]
                    else:
                        found[g] = jnp.take_along_axis(a[g], tone + (2 * j + c), axis=1, mode="promise_in_bounds")
                panel.append(found)
        for j in range(start, start + size):
            at, c = j % 8, j - start
            real, imag = panel[2 * c], panel[2 * c + 1]
            top = real[home][at : at + 1, :]
            by_row[home] = jnp.where(row == at, lax.rsqrt(top), by_row[home])
            if j == users - 1:
                break
            inverse = 1.0 / top
            pivots = [(x, ix, x[home][at : at + 1, :] * inverse, ix[home][at : at + 1, :] * inverse) for x, ix in ((a, ia), (q, iq))]
            later = [
                (d, real[home][at + d - c : at + d - c + 1, :] * inverse, imag[home][at + d - c : at + d - c + 1, :] * inverse)
                for d in range(c + 1, size)
            ]
            for g in range(home + (at == 7), groups):
                fr, fi = real[g], imag[g]
                if g == home:
                    fr, fi = jnp.where(row > at, fr, 0.0), jnp.where(row > at, fi, 0.0)
                for d, x, y in later:
                    panel[2 * d][g] = panel[2 * d][g] - (fr * x + fi * y)
                    panel[2 * d + 1][g] = panel[2 * d + 1][g] - (fi * x - fr * y)
                for x, ix, pivot_row, turned_row in pivots:
                    x[g] = x[g] - (fr * pivot_row + fi * turned_row)
                    ix[g] = ix[g] - (fr * turned_row - fi * pivot_row)
    upper = []
    for g in range(groups):
        diagonal = 2 * (row + 8 * g)
        keep = (lanes % width >= diagonal) & (lanes % width != diagonal + 1)
        upper.append(jnp.where(keep, a[g] * (by_row[g] * constellation_norm), 0.0))
    return upper, [x * scale for x, scale in zip(q, by_row)]


def kernel(
    dims, noise_any, gains_ref, samples_ref, branches_any, out_ref,
    noise_ref, branches_ref, held, raw, part, came, points, packed, taken,
    small_sem, load_sem, send_sem, recv_sem, usend_sem, urecv_sem,
):
    clusters, bands, users, symbols, share, mine_t, pieces = dims
    me, band = lax.axis_index("chain"), lax.axis_index("par")

    barrier = pltpu.get_barrier_semaphore()
    for k in range(1, clusters):
        pl.semaphore_signal(barrier, inc=1, device_id={"chain": lax.rem(me + k, clusters)}, device_id_type=MESH)
    for k in range(1, bands):
        pl.semaphore_signal(barrier, inc=1, device_id={"par": lax.rem(band + k, bands)}, device_id_type=MESH)

    far, mid = clusters // 2, clusters // 4
    order = list(range(clusters - 1, -1, -1))
    peers = {}
    for k in order:
        peers[k], bit = me - me, 1
        while bit < clusters:
            digit = lax.rem(me // bit, 2)
            peers[k] = peers[k] + bit * (1 - digit if (k // bit) % 2 else digit)
            bit *= 2
    loads = {}
    for k in order:
        tones = pl.ds(peers[k] * share, share)
        loads[k] = (
            pltpu.make_async_copy(
                gains_ref.at[0, tones], held.at[k, :, pl.ds(0, 2 * users)], load_sem.at[0, k]
            ),
            pltpu.make_async_copy(
                samples_ref.at[0, tones], held.at[k, :, pl.ds(2 * users, 2 * symbols)], load_sem.at[1, k]
            ),
        )
        for copy in loads[k]:
            copy.start()

    small = (
        pltpu.make_async_copy(noise_any, noise_ref, small_sem.at[0]),
        pltpu.make_async_copy(branches_any, branches_ref, small_sem.at[1]),
    )
    for copy in small:
        copy.start()
    half, quarter, width = users // 2, users // 4, 2 * users
    tail = share * half + quarter
    compact = 2 * symbols <= users
    at, edge8 = iota((half, LANES), 1), iota((quarter, LANES), 1) // users
    even = iota((users, LANES), 1) % 2 == 0
    sends = []

    def fold(number, k, products):
        lower = []
        for s, product in enumerate(products):
            slot = (number * share + s) % raw.shape[0]
            raw[slot, :, : width + 2 * symbols] = product
            on_even = raw[slot, pl.ds(0, users, stride=2), :]
            on_odd = raw[slot, pl.ds(1, users, stride=2), :]
            whole = pair_swap(on_odd) + jnp.where(even, on_even, -on_even)
            lower.append(whole[half:])
            upper = whole[:half]
            if compact:
                upper = jnp.where(at < 3 * users, upper, pltpu.roll(whole[half:], users, 1))
            part[k, s * half : (s + 1) * half] = upper
        part[k, share * half : tail] = jnp.where(
            edge8 == 0, pltpu.roll(lower[1][:quarter], 3 * users, 1),
            jnp.where(
                edge8 == 1, lower[0][quarter:],
                jnp.where(edge8 == 2, pltpu.roll(lower[0][:quarter], users, 1), pltpu.roll(lower[1][quarter:], width, 1)),
            ),
        )
        if not compact:
            part[k, tail:] = jnp.where(at < width, pltpu.roll(lower[0], width, 1), lower[1])
        if k:
            if number == 0:
                pl.semaphore_wait(barrier, clusters + bands - 2)
            copy = pltpu.make_async_remote_copy(
                src_ref=part.at[k], dst_ref=came.at[k], send_sem=send_sem.at[k], recv_sem=recv_sem.at[k],
                device_id={"chain": peers[k]}, device_id_type=MESH,
            )
            copy.start()
            sends.append(copy)

    raw[...] = jnp.zeros_like(raw)
    waiting = []
    numbered = list(enumerate(order))
    for lot in [numbered[:1]] + [numbered[i : i + 2] for i in range(1, clusters, 2)]:
        fresh = []
        for number, k in lot:
            for copy in loads[k]:
                copy.wait()
        for number, k in lot:
            products = []
            for s in range(share):
                both = held[k, s]
                products.append(lax.dot_general(both[:width], both, NT, preferred_element_type=jnp.float32))
            fresh.append((number, k, products))
        for chunk in waiting:
            fold(*chunk)
        waiting = fresh
    for chunk in waiting:
        fold(*chunk)

    for copy in small:
        copy.wait()
    rows = pieces * mine_t
    source, target = iota((2 * LANES, 4 * LANES), 0), iota((2 * LANES, 4 * LANES), 1)
    place = target % (2 * LANES)
    user, quadrature, off = place // 2, place % 2, target // (2 * LANES)
    entry = jnp.where(source == user + LANES * ((quadrature + off) % 2), 1.0, 0.0)
    entry = jnp.where(off * quadrature == 1, -entry, entry).astype(jnp.bfloat16)
    marks = jnp.concatenate(
        [
            branches_ref[b, s, :, LANES * r : LANES * (r + 1)]
            for b in range(bands) for s in range(share) for r in range(pieces)
        ],
        axis=0,
    )
    pair = jnp.concatenate(
        [(2 * (marks & 7) - 7).astype(jnp.float32), (2 * (marks >> 3) - 7).astype(jnp.float32)], axis=1
    ).astype(jnp.bfloat16)
    woven = jnp.dot(pair, entry, preferred_element_type=jnp.float32).astype(jnp.bfloat16)
    for b in range(bands):
        for s in range(share):
            first = (b * share + s) * rows
            for h in range(2):
                for o in range(2):
                    points[b, s, pl.ds((2 * h + o) * rows, rows), :] = woven[
                        first : first + rows, LANES * (2 * o + h) : LANES * (2 * o + h + 1)
                    ]

    noises = [
        jnp.sum(jnp.where(iota((1, bands), 1) == band, noise_ref[s : s + 1, :], 0.0), axis=1, keepdims=True)
        for s in range(share)
    ]
    row, lanes, extra = iota((8, LANES), 0), iota((8, LANES), 1), 2 * mine_t
    noise = jnp.where(lanes >= width, noises[1], noises[0])
    for copy in sends:
        copy.wait_recv()
    total = part[0]
    for k in range(1, clusters):
        total = total + came[k]
    tile, ups = total[share * half : tail], [total[s * half : (s + 1) * half] for s in range(share)]
    inside = iota((quarter, LANES), 1) % width >= users
    above = jnp.where(at < width, ups[0], pltpu.roll(ups[1], width, 1))
    below = [jnp.where(inside, x, 0.0) for x in (pltpu.roll(tile, 3 * users, 1), tile)]
    seen = [jnp.where(at < width, pltpu.roll(ups[0], width, 1), ups[1])]
    if compact:
        seen.append(jnp.where(at < width, pltpu.roll(ups[0], users, 1), pltpu.roll(ups[1], 3 * users, 1)))
    else:
        seen.append(total[tail:])
    seen = [jnp.where(at % width < 2 * symbols, x, 0.0) for x in seen]
    lines = [above[:8], above[8:]] + below
    for g in range(users // 8):
        lines[g] = jnp.where(lanes % width == 2 * (row + 8 * g), lines[g] + noise, lines[g])
    upper, rotated = eliminate(lines, [x[8 * i : 8 * i + 8] for x in seen for i in range(half // 8)], users)
    corner = jnp.where(inside, upper[3], pltpu.roll(upper[2], 3 * users, 1))
    for b in range(bands):
        z = jnp.zeros_like(corner)
        for g in range(users // 8):
            shift = extra * (g - b) % LANES
            z = jnp.where(lanes % width // extra == g, pltpu.roll(rotated[g], shift, 1) if shift else rotated[g], z)
        packed[b, :8] = upper[0]
        packed[b, 8:half] = upper[1]
        packed[b, half : half + quarter] = corner
        packed[b, half + quarter :] = z
    near = []
    inner = jnp.minimum(band, bands - 1 - band)
    outward = jnp.where(2 * band < bands - 1, 1, -1)
    for i in range(1, bands):
        both_sides = (i + 1) // 2 if i % 2 else -(i // 2)
        near.append(band + jnp.where(i <= 2 * inner, both_sides, outward * (i - inner)))
    usends = []
    for i in range(bands - 1, 0, -1):
        peer = near[i - 1]
        copy = pltpu.make_async_remote_copy(
            src_ref=packed.at[peer], dst_ref=taken.at[band], send_sem=usend_sem.at[i], recv_sem=urecv_sem.at[band],
            device_id={"par": peer}, device_id_type=MESH,
        )
        copy.start()
        usends.append(copy)

    r, c = iota((4 * rows, LANES), 0), iota((4 * rows, LANES), 1)
    is_off = (r // rows) % 2
    chosen = jnp.where(c % extra == 2 * (r % mine_t) + is_off, (2 * is_off - 1).astype(jnp.float32), 0.0).astype(jnp.bfloat16)
    sr, sc = iota((width, LANES), 0), iota((width, LANES), 1)
    suffix = [
        jnp.where((sr // users + 2 * h == sc // users) & (sr % users >= sc % users), 1.0 / users, 0.0).astype(jnp.bfloat16)
        for h in range(2)
    ]
    for i in range(bands):
        b = band if i == 0 else near[i - 1]
        if i:
            pltpu.make_async_remote_copy(
                src_ref=packed.at[b], dst_ref=taken.at[b], send_sem=usend_sem.at[i], recv_sem=urecv_sem.at[b],
                device_id={"par": b}, device_id_type=MESH,
            ).wait_recv()
        box = taken if i else packed
        top, corner = box[b, :half], box[b, half : half + quarter]
        straight = [(top, corner, pltpu.roll(corner, users, 1))]
        straight.append((pltpu.roll(top, width, 1), pltpu.roll(corner, width, 1), pltpu.roll(corner, 3 * users, 1)))
        z = box[b, half + quarter :]
        rests = []
        side, edge = iota(top.shape, 1) // width, iota(corner.shape, 1) // users
        for s in range(share):
            weights = []
            for e in range(2):
                above, fourth, third = straight[(s + e) % 2]
                weights += [
                    jnp.where(side == e, above, 0.0),
                    jnp.where(edge == 2 * e + 1, third, 0.0),
                    jnp.where(edge == 2 * e + 1, fourth, 0.0),
                ]
            own = [jnp.where(lanes // extra == width * s // extra + g, z, 0.0) for g in range(users // 8)]
            high, low = split(
                jnp.concatenate([jnp.concatenate(weights, axis=0), jnp.concatenate(own + own, axis=0)], axis=1)
            )
            p = jnp.concatenate([points[b, s], chosen], axis=1)
            rest = lax.dot_general(p, high, NT, preferred_element_type=jnp.float32) + lax.dot_general(
                p, low, NT, preferred_element_type=jnp.float32
            )
            rests.append(rest)
        for s, rest in enumerate(rests):
            result = None
            for h in range(2):
                on, off = rest[2 * h * rows : (2 * h + 1) * rows], rest[(2 * h + 1) * rows : (2 * h + 2) * rows]
                for term in split(on * on + off * off):
                    step = jnp.dot(term, suffix[h], preferred_element_type=jnp.float32)
                    result = step if result is None else result + step
            for r in range(pieces):
                out_ref[b, s, :, LANES * r : LANES * (r + 1)] = result[mine_t * r : mine_t * (r + 1)]
    for copy in sends + usends:
        copy.wait_send()


def local(propagation_gains, observed_samples, disturbance_variance, retained_branches):
    clusters, bands = lax.axis_size("chain"), lax.axis_size("par")
    _, tones, double_users, antennas = propagation_gains.shape
    users, symbols = double_users // 2, observed_samples.shape[2] // 2
    share, mine_t = tones // clusters, symbols // bands
    pieces = retained_branches.shape[-1] // LANES
    assert share == 2 and 4 * users == LANES and 4 * mine_t <= users // 2
    dims = (clusters, bands, users, symbols, share, mine_t, pieces)
    lines = share * users // 2 + users // 4 + (0 if 2 * symbols <= users else users // 2)
    f32, bf16 = jnp.float32, jnp.bfloat16
    vmem, dma = pltpu.VMEM, pltpu.SemaphoreType.DMA
    return pl.pallas_call(
        functools.partial(kernel, dims),
        out_shape=pltpu.VMEM(retained_branches.shape, f32),
        in_specs=[
            pl.BlockSpec(memory_space=pl.ANY),
            pl.BlockSpec(memory_space=pl.ANY),
            pl.BlockSpec(memory_space=pl.ANY),
            pl.BlockSpec(memory_space=pl.ANY),
        ],
        out_specs=pl.BlockSpec(memory_space=pltpu.VMEM),
        scratch_shapes=[
            vmem(disturbance_variance.shape[::-1], f32),
            vmem(retained_branches.shape, jnp.int32),
            vmem((clusters, share, 2 * (users + symbols), antennas), bf16),
            vmem((4, 2 * users, LANES), f32),
            vmem((clusters, lines, LANES), f32),
            vmem((clusters, lines, LANES), f32),
            vmem((bands, share, 4 * pieces * mine_t, LANES), bf16),
            vmem((bands, users, LANES), f32),
            vmem((bands, users, LANES), f32),
            dma((2,)), dma((2, clusters)), dma((clusters,)), dma((clusters,)), dma((bands,)), dma((bands,)),
        ],
        compiler_params=pltpu.CompilerParams(collective_id=0, has_side_effects=True),
        name="detect",
    )(*(
        pltpu.with_memory_space_constraint(x, pltpu.HBM)
        for x in (disturbance_variance.T, propagation_gains, observed_samples, retained_branches)
    ))


def solution(mesh):
    placed = (
        P("par", None, None, "chain"),
        P("par", None, None, "chain"),
        P(None, "chain"),
        P(None, "chain", "par", None),
    )
    return jax.shard_map(
        local, mesh=mesh, in_specs=placed, out_specs=P(None, "chain", "par", None), check_vma=False
    )
```

```python
import functools
import jax
import jax.numpy as jnp
from jax import lax
from jax.experimental import pallas as pl
from jax.experimental.pallas import tpu as pltpu
from jax.sharding import PartitionSpec as P

constellation_norm = 1.0 / 42.0**0.5
LANES = 128
MESH = pl.DeviceIdType.MESH
NT = (((1,), (1,)), ((), ()))


def iota(shape, dim):
    return lax.broadcasted_iota(jnp.int32, shape, dim)


def panels(users):
    wide = users // 2
    return [(j, 4) for j in range(0, wide, 4)] + [(j, 8) for j in range(wide, users, 8)]


def split(x):
    high = x.astype(jnp.bfloat16)
    return high, (x - high.astype(jnp.float32)).astype(jnp.bfloat16)


def pair_swap(x):
    even = iota(x.shape, 1) % 2 == 0
    return jnp.where(even, pltpu.roll(x, LANES - 1, 1), pltpu.roll(x, 1, 1))


def eliminate(a, q, users):
    groups, width = users // 8, 2 * users
    row, lanes = iota((8, LANES), 0), iota((8, LANES), 1)
    tone = jnp.where(lanes >= width, width, 0)
    ia, iq = [[jnp.where(lanes % 2 == 1, pair_swap(p), -pair_swap(p)) for p in x] for x in (a, q)]
    by_row = [jnp.ones((8, LANES), jnp.float32) for _ in range(groups)]
    for start, size in panels(users):
        home = start // 8
        panel = []
        for j in range(start, start + size):
            pivot = jnp.broadcast_to(a[home][j % 8 : j % 8 + 1, :], (8, LANES))
            for c in range(2):
                found = {}
                for g in range(home, groups):
                    if start < users // 2 <= 8 * g:
                        ones = [
                            jnp.sum(jnp.where(lanes == t * width + 2 * (row + 8 * g) + c, pivot, 0.0), axis=1, keepdims=True)
                            for t in range(2)
                        ]
                        found[g] = jnp.where(lanes >= width, ones[1], ones[0])
                        if c:
                            found[g] = -found[g]
                    else:
                        found[g] = jnp.take_along_axis(a[g], tone + (2 * j + c), axis=1, mode="promise_in_bounds")
                panel.append(found)
        for j in range(start, start + size):
            at, c = j % 8, j - start
            real, imag = panel[2 * c], panel[2 * c + 1]
            top = real[home][at : at + 1, :]
            by_row[home] = jnp.where(row == at, lax.rsqrt(top), by_row[home])
            if j == users - 1:
                break
            inverse = 1.0 / top
            pivots = [(x, ix, x[home][at : at + 1, :] * inverse, ix[home][at : at + 1, :] * inverse) for x, ix in ((a, ia), (q, iq))]
            later = [
                (d, real[home][at + d - c : at + d - c + 1, :] * inverse, imag[home][at + d - c : at + d - c + 1, :] * inverse)
                for d in range(c + 1, size)
            ]
            for g in range(home + (at == 7), groups):
                fr, fi = real[g], imag[g]
                if g == home:
                    fr, fi = jnp.where(row > at, fr, 0.0), jnp.where(row > at, fi, 0.0)
                for d, x, y in later:
                    panel[2 * d][g] = panel[2 * d][g] - (fr * x + fi * y)
                    panel[2 * d + 1][g] = panel[2 * d + 1][g] - (fi * x - fr * y)
                for x, ix, pivot_row, turned_row in pivots:
                    x[g] = x[g] - (fr * pivot_row + fi * turned_row)
                    ix[g] = ix[g] - (fr * turned_row - fi * pivot_row)
    upper = []
    for g in range(groups):
        diagonal = 2 * (row + 8 * g)
        keep = (lanes % width >= diagonal) & (lanes % width != diagonal + 1)
        upper.append(jnp.where(keep, a[g] * (by_row[g] * constellation_norm), 0.0))
    return upper, [x * scale for x, scale in zip(q, by_row)]


def kernel(
    dims, noise_any, gains_ref, samples_ref, branches_any, out_ref,
    noise_ref, branches_ref, held, raw, part, came, points, packed, taken,
    small_sem, load_sem, send_sem, recv_sem, usend_sem, urecv_sem,
):
    clusters, bands, users, symbols, share, mine_t, pieces = dims
    me, band = lax.axis_index("chain"), lax.axis_index("par")

    barrier = pltpu.get_barrier_semaphore()
    for k in range(1, clusters):
        pl.semaphore_signal(barrier, inc=1, device_id={"chain": lax.rem(me + k, clusters)}, device_id_type=MESH)
    for k in range(1, bands):
        pl.semaphore_signal(barrier, inc=1, device_id={"par": lax.rem(band + k, bands)}, device_id_type=MESH)

    far, mid = clusters // 2, clusters // 4
    order = list(range(clusters - 1, -1, -1))
    peers = {}
    for k in order:
        peers[k], bit = me - me, 1
        while bit < clusters:
            digit = lax.rem(me // bit, 2)
            peers[k] = peers[k] + bit * (1 - digit if (k // bit) % 2 else digit)
            bit *= 2
    loads = {}
    for k in order:
        tones = pl.ds(peers[k] * share, share)
        loads[k] = (
            pltpu.make_async_copy(
                gains_ref.at[0, tones], held.at[k, :, pl.ds(0, 2 * users)], load_sem.at[k]
            ),
            pltpu.make_async_copy(
                samples_ref.at[0, tones], held.at[k, :, pl.ds(2 * users, 2 * symbols)], load_sem.at[k]
            ),
        )
        for copy in loads[k]:
            copy.start()

    small = (
        pltpu.make_async_copy(noise_any, noise_ref, small_sem.at[0]),
        pltpu.make_async_copy(branches_any, branches_ref, small_sem.at[1]),
    )
    for copy in small:
        copy.start()
    half, quarter, width = users // 2, users // 4, 2 * users
    tail = share * half + quarter
    compact = 2 * symbols <= users
    at, edge8 = iota((half, LANES), 1), iota((quarter, LANES), 1) // users
    even = iota((users, LANES), 1) % 2 == 0
    sends, ready = [], []

    def fold(number, k, products):
        lower = []
        for s, product in enumerate(products):
            slot = (number * share + s) % raw.shape[0]
            raw[slot, :, : width + 2 * symbols] = product
            on_even = raw[slot, pl.ds(0, users, stride=2), :]
            on_odd = raw[slot, pl.ds(1, users, stride=2), :]
            whole = pair_swap(on_odd) + jnp.where(even, on_even, -on_even)
            lower.append(whole[half:])
            upper, bottom = whole[:half], whole[half:]
            if s:
                upper = pltpu.roll(upper, width, 1)
                if compact:
                    upper = jnp.where((at >= users) & (at < width), pltpu.roll(bottom, 3 * users, 1), upper)
            elif compact:
                upper = jnp.where(at < 3 * users, upper, pltpu.roll(bottom, users, 1))
            part[k, s * half : (s + 1) * half] = upper
        part[k, share * half : tail] = jnp.where(
            edge8 == 0, pltpu.roll(lower[1][:quarter], 3 * users, 1),
            jnp.where(
                edge8 == 1, lower[0][quarter:],
                jnp.where(edge8 == 2, pltpu.roll(lower[0][:quarter], users, 1), pltpu.roll(lower[1][quarter:], width, 1)),
            ),
        )
        if not compact:
            part[k, tail:] = jnp.where(at < width, pltpu.roll(lower[0], width, 1), lower[1])
        if k:
            ready.append(
                pltpu.make_async_remote_copy(
                    src_ref=part.at[k], dst_ref=came.at[k], send_sem=send_sem.at[0], recv_sem=recv_sem.at[0],
                    device_id={"chain": peers[k]}, device_id_type=MESH,
                )
            )

    def post(last):
        if ready and (sends or last >= 0):
            if not sends:
                pl.semaphore_wait(barrier, clusters + bands - 2)
            for copy in ready:
                copy.start()
            sends.extend(ready)
            ready.clear()

    raw[...] = jnp.zeros_like(raw)
    waiting = []
    numbered = list(enumerate(order))
    for lot in [numbered[:1]] + [numbered[i : i + 2] for i in range(1, clusters, 2)]:
        fresh = []
        for number, k in lot:
            pltpu.make_async_copy(held.at[k], held.at[k], load_sem.at[k]).wait()
        for number, k in lot:
            products = []
            for s in range(share):
                both = held[k, s]
                products.append(lax.dot_general(both[:width], both, NT, preferred_element_type=jnp.float32))
            fresh.append((number, k, products))
        for chunk in waiting:
            fold(*chunk)
        post(lot[0][0] - 1)
        waiting = fresh
    for chunk in waiting:
        fold(*chunk)
    post(clusters)

    for copy in small:
        copy.wait()
    rows = pieces * mine_t
    source, target = iota((2 * LANES, 4 * LANES), 0), iota((2 * LANES, 4 * LANES), 1)
    place = target % (2 * LANES)
    user, quadrature, off = place // 2, place % 2, target // (2 * LANES)
    entry = jnp.where(source == user + LANES * ((quadrature + off) % 2), 1.0, 0.0)
    entry = jnp.where(off * quadrature == 1, -entry, entry).astype(jnp.bfloat16)
    marks = jnp.concatenate(
        [
            branches_ref[b, s, :, LANES * r : LANES * (r + 1)]
            for b in range(bands) for s in range(share) for r in range(pieces)
        ],
        axis=0,
    )
    pair = jnp.concatenate(
        [(2 * (marks & 7) - 7).astype(jnp.float32), (2 * (marks >> 3) - 7).astype(jnp.float32)], axis=1
    ).astype(jnp.bfloat16)
    woven = jnp.dot(pair, entry, preferred_element_type=jnp.float32).astype(jnp.bfloat16)
    for b in range(bands):
        for s in range(share):
            first = (b * share + s) * rows
            for h in range(2):
                for o in range(2):
                    points[b, s, pl.ds((2 * h + o) * rows, rows), :] = woven[
                        first : first + rows, LANES * (2 * o + h) : LANES * (2 * o + h + 1)
                    ]

    noises = [
        jnp.sum(jnp.where(iota((1, bands), 1) == band, noise_ref[s : s + 1, :], 0.0), axis=1, keepdims=True)
        for s in range(share)
    ]
    row, lanes, extra = iota((8, LANES), 0), iota((8, LANES), 1), 2 * mine_t
    noise = jnp.where(lanes >= width, noises[1], noises[0])
    every = pltpu.make_async_remote_copy(
        src_ref=part.at[pl.ds(1, clusters - 1)], dst_ref=came.at[pl.ds(1, clusters - 1)], send_sem=send_sem.at[0],
        recv_sem=recv_sem.at[0], device_id={"chain": peers[1]}, device_id_type=MESH,
    )
    every.wait_recv()
    total = part[0]
    for k in range(1, clusters):
        total = total + came[k]
    tile, ups = total[share * half : tail], [total[s * half : (s + 1) * half] for s in range(share)]
    inside = iota((quarter, LANES), 1) % width >= users
    above, heard = jnp.where(at < width, ups[0], ups[1]), jnp.where(at < width, ups[1], ups[0])
    below = [jnp.where(inside, x, 0.0) for x in (pltpu.roll(tile, 3 * users, 1), tile)]
    seen = [pltpu.roll(heard, width, 1), pltpu.roll(heard, users, 1) if compact else total[tail:]]
    seen = [jnp.where(at % width < 2 * symbols, x, 0.0) for x in seen]
    lines = [above[:8], above[8:]] + below
    for g in range(users // 8):
        lines[g] = jnp.where(lanes % width == 2 * (row + 8 * g), lines[g] + noise, lines[g])
    upper, rotated = eliminate(lines, [x[8 * i : 8 * i + 8] for x in seen for i in range(half // 8)], users)
    corner = jnp.where(inside, upper[3], pltpu.roll(upper[2], 3 * users, 1))
    for b in range(bands):
        z = jnp.zeros_like(corner)
        for g in range(users // 8):
            slot = (b + g + 1 - users // 8) % (width // extra)
            shift = extra * (slot - b) % LANES
            z = jnp.where(lanes % width // extra == slot, pltpu.roll(rotated[g], shift, 1) if shift else rotated[g], z)
        packed[b, :8] = upper[0]
        packed[b, 8:half] = upper[1]
        packed[b, half : half + quarter] = corner
        packed[b, half + quarter :] = z
    near = []
    inner = jnp.minimum(band, bands - 1 - band)
    outward = jnp.where(2 * band < bands - 1, 1, -1)
    for i in range(1, bands):
        both_sides = (i + 1) // 2 if i % 2 else -(i // 2)
        near.append(band + jnp.where(i <= 2 * inner, both_sides, outward * (i - inner)))
    usends = []
    for i in range(bands - 1, 0, -1):
        peer = near[i - 1]
        copy = pltpu.make_async_remote_copy(
            src_ref=packed.at[peer], dst_ref=taken.at[band], send_sem=usend_sem.at[0], recv_sem=urecv_sem.at[band],
            device_id={"par": peer}, device_id_type=MESH,
        )
        copy.start()
        usends.append(copy)

    r, c = iota((4 * rows, LANES), 0), iota((4 * rows, LANES), 1)
    is_off = (r // rows) % 2
    chosen = jnp.where(c % extra == 2 * (r % mine_t) + is_off, (2 * is_off - 1).astype(jnp.float32), 0.0).astype(jnp.bfloat16)
    slots = [lax.rem(band + g + 1 + (width // extra) - users // 8, width // extra) for g in range(users // 8)]
    sr, sc = iota((width, LANES), 0), iota((width, LANES), 1)
    suffix = [
        jnp.where((sr // users + 2 * h == sc // users) & (sr % users >= sc % users), 1.0 / users, 0.0).astype(jnp.bfloat16)
        for h in range(2)
    ]
    for i in range(bands):
        b = band if i == 0 else near[i - 1]
        if i:
            pltpu.make_async_remote_copy(
                src_ref=packed.at[b], dst_ref=taken.at[b], send_sem=usend_sem.at[0], recv_sem=urecv_sem.at[b],
                device_id={"par": b}, device_id_type=MESH,
            ).wait_recv()
        box = taken if i else packed
        top, corner = box[b, :half], box[b, half : half + quarter]
        straight = [(top, corner, pltpu.roll(corner, users, 1))]
        straight.append((pltpu.roll(top, width, 1), pltpu.roll(corner, width, 1), pltpu.roll(corner, 3 * users, 1)))
        z = box[b, half + quarter :]
        rests = []
        side, edge = iota(top.shape, 1) // width, iota(corner.shape, 1) // users
        for s in range(share):
            weights = []
            for e in range(2):
                above, fourth, third = straight[(s + e) % 2]
                weights += [
                    jnp.where(side == e, above, 0.0),
                    jnp.where(edge == 2 * e + 1, third, 0.0),
                    jnp.where(edge == 2 * e + 1, fourth, 0.0),
                ]
            own = [
                jnp.where(lanes // extra == width * s // extra + slots[g], z, 0.0) for g in range(users // 8)
            ]
            high, low = split(
                jnp.concatenate([jnp.concatenate(weights, axis=0), jnp.concatenate(own + own, axis=0)], axis=1)
            )
            p = jnp.concatenate([points[b, s], chosen], axis=1)
            rest = lax.dot_general(p, high, NT, preferred_element_type=jnp.float32) + lax.dot_general(
                p, low, NT, preferred_element_type=jnp.float32
            )
            rests.append(rest)
        for s, rest in enumerate(rests):
            result = None
            for h in range(2):
                on, off = rest[2 * h * rows : (2 * h + 1) * rows], rest[(2 * h + 1) * rows : (2 * h + 2) * rows]
                for term in split(on * on + off * off):
                    step = jnp.dot(term, suffix[h], preferred_element_type=jnp.float32)
                    result = step if result is None else result + step
            for r in range(pieces):
                out_ref[b, s, :, LANES * r : LANES * (r + 1)] = result[mine_t * r : mine_t * (r + 1)]
    every.wait_send()
    pltpu.make_async_remote_copy(
        src_ref=packed.at[pl.ds(1, bands - 1)], dst_ref=taken.at[pl.ds(1, bands - 1)], send_sem=usend_sem.at[0],
        recv_sem=urecv_sem.at[0], device_id={"par": near[0]}, device_id_type=MESH,
    ).wait_send()


def local(propagation_gains, observed_samples, disturbance_variance, retained_branches):
    clusters, bands = lax.axis_size("chain"), lax.axis_size("par")
    _, tones, double_users, antennas = propagation_gains.shape
    users, symbols = double_users // 2, observed_samples.shape[2] // 2
    share, mine_t = tones // clusters, symbols // bands
    pieces = retained_branches.shape[-1] // LANES
    assert share == 2 and 4 * users == LANES and 4 * mine_t <= users // 2
    dims = (clusters, bands, users, symbols, share, mine_t, pieces)
    lines = share * users // 2 + users // 4 + (0 if 2 * symbols <= users else users // 2)
    f32, bf16 = jnp.float32, jnp.bfloat16
    vmem, dma = pltpu.VMEM, pltpu.SemaphoreType.DMA
    return pl.pallas_call(
        functools.partial(kernel, dims),
        out_shape=pltpu.VMEM(retained_branches.shape, f32),
        in_specs=[
            pl.BlockSpec(memory_space=pl.ANY),
            pl.BlockSpec(memory_space=pl.ANY),
            pl.BlockSpec(memory_space=pl.ANY),
            pl.BlockSpec(memory_space=pl.ANY),
        ],
        out_specs=pl.BlockSpec(memory_space=pltpu.VMEM),
        scratch_shapes=[
            vmem(disturbance_variance.shape[::-1], f32),
            vmem(retained_branches.shape, jnp.int32),
            vmem((clusters, share, 2 * (users + symbols), antennas), bf16),
            vmem((4, 2 * users, LANES), f32),
            vmem((clusters, lines, LANES), f32),
            vmem((clusters, lines, LANES), f32),
            vmem((bands, share, 4 * pieces * mine_t, LANES), bf16),
            vmem((bands, users, LANES), f32),
            vmem((bands, users, LANES), f32),
            dma((2,)), dma((clusters,)), dma((1,)), dma((1,)), dma((1,)), dma((bands,)),
        ],
        compiler_params=pltpu.CompilerParams(collective_id=0, has_side_effects=True),
        name="detect",
    )(*(
        pltpu.with_memory_space_constraint(x, pltpu.HBM)
        for x in (disturbance_variance.T, propagation_gains, observed_samples, retained_branches)
    ))


def solution(mesh):
    placed = (
        P("par", None, None, "chain"),
        P("par", None, None, "chain"),
        P(None, "chain"),
        P(None, "chain", "par", None),
    )
    return jax.shard_map(
        local, mesh=mesh, in_specs=placed, out_specs=P(None, "chain", "par", None), check_vma=False
    )
```

```python
import functools
import jax
import jax.numpy as jnp
from jax import lax
from jax.experimental import pallas as pl
from jax.experimental.pallas import tpu as pltpu
from jax.sharding import PartitionSpec as P

constellation_norm = 1.0 / 42.0**0.5
LANES = 128
MESH = pl.DeviceIdType.MESH
NT = (((1,), (1,)), ((), ()))


def iota(shape, dim):
    return lax.broadcasted_iota(jnp.int32, shape, dim)


def panels(users):
    return [(0, 4), (4, 4)] + [(j, 8) for j in range(8, users, 8)]


def split(x):
    high = x.astype(jnp.bfloat16)
    return high, (x - high.astype(jnp.float32)).astype(jnp.bfloat16)


def pair_swap(x):
    even = iota(x.shape, 1) % 2 == 0
    return jnp.where(even, pltpu.roll(x, LANES - 1, 1), pltpu.roll(x, 1, 1))


def eliminate(a, q, users):
    groups, width = users // 8, 2 * users
    row, lanes = iota((8, LANES), 0), iota((8, LANES), 1)
    tone = jnp.where(lanes >= width, width, 0)
    ia, iq = [[jnp.where(lanes % 2 == 1, pair_swap(p), -pair_swap(p)) for p in x] for x in (a, q)]
    by_row = [jnp.ones((8, LANES), jnp.float32) for _ in range(groups)]
    for start, size in panels(users):
        home = start // 8
        panel = []
        for j in range(start, start + size):
            pivot = jnp.broadcast_to(a[home][j % 8 : j % 8 + 1, :], (8, LANES))
            for c in range(2):
                found = {}
                for g in range(home, groups):
                    if start < users // 2 <= 8 * g:
                        ones = [
                            jnp.sum(jnp.where(lanes == t * width + 2 * (row + 8 * g) + c, pivot, 0.0), axis=1, keepdims=True)
                            for t in range(2)
                        ]
                        found[g] = jnp.where(lanes >= width, ones[1], ones[0])
                        if c:
                            found[g] = -found[g]
                    else:
                        found[g] = jnp.take_along_axis(a[g], tone + (2 * j + c), axis=1, mode="promise_in_bounds")
                panel.append(found)
        for j in range(start, start + size):
            at, c = j % 8, j - start
            real, imag = panel[2 * c], panel[2 * c + 1]
            top = real[home][at : at + 1, :]
            by_row[home] = jnp.where(row == at, lax.rsqrt(top), by_row[home])
            if j == users - 1:
                break
            inverse = 1.0 / top
            pivots = [(x, ix, x[home][at : at + 1, :] * inverse, ix[home][at : at + 1, :] * inverse) for x, ix in ((a, ia), (q, iq))]
            later = [
                (d, real[home][at + d - c : at + d - c + 1, :] * inverse, imag[home][at + d - c : at + d - c + 1, :] * inverse)
                for d in range(c + 1, size)
            ]
            for g in range(home + (at == 7), groups):
                fr, fi = real[g], imag[g]
                if g == home:
                    fr, fi = jnp.where(row > at, fr, 0.0), jnp.where(row > at, fi, 0.0)
                for d, x, y in later:
                    panel[2 * d][g] = panel[2 * d][g] - (fr * x + fi * y)
                    panel[2 * d + 1][g] = panel[2 * d + 1][g] - (fi * x - fr * y)
                for x, ix, pivot_row, turned_row in pivots:
                    x[g] = x[g] - (fr * pivot_row + fi * turned_row)
                    ix[g] = ix[g] - (fr * turned_row - fi * pivot_row)
    upper = []
    for g in range(groups):
        diagonal = 2 * (row + 8 * g)
        keep = (lanes % width >= diagonal) & (lanes % width != diagonal + 1)
        upper.append(jnp.where(keep, a[g] * (by_row[g] * constellation_norm), 0.0))
    return upper, [x * scale for x, scale in zip(q, by_row)]


def kernel(
    dims, noise_any, gains_ref, samples_ref, branches_any, out_ref,
    noise_ref, branches_ref, held, raw, part, came, points, packed, taken,
    small_sem, load_sem, send_sem, recv_sem, usend_sem, urecv_sem,
):
    clusters, bands, users, symbols, share, mine_t, pieces = dims
    me, band = lax.axis_index("chain"), lax.axis_index("par")

    far, mid = clusters // 2, clusters // 4
    order = list(range(clusters - 1, -1, -1))
    peers = {}
    for k in order:
        peers[k], bit = me - me, 1
        while bit < clusters:
            digit = lax.rem(me // bit, 2)
            peers[k] = peers[k] + bit * (1 - digit if (k // bit) % 2 else digit)
            bit *= 2
    def load(k):
        tones = pl.ds(peers[k] * share, share)
        pltpu.make_async_copy(gains_ref.at[0, tones], held.at[k, :, pl.ds(0, 2 * users)], load_sem.at[k]).start()
        pltpu.make_async_copy(
            samples_ref.at[0, tones], held.at[k, :, pl.ds(2 * users, 2 * symbols)], load_sem.at[k]
        ).start()

    for k in order[:clusters]:
        load(k)
    barrier = pltpu.get_barrier_semaphore()
    for k in range(1, clusters):
        pl.semaphore_signal(barrier, inc=1, device_id={"chain": lax.rem(me + k, clusters)}, device_id_type=MESH)
    for k in range(1, bands):
        pl.semaphore_signal(barrier, inc=1, device_id={"par": lax.rem(band + k, bands)}, device_id_type=MESH)

    small = (
        pltpu.make_async_copy(noise_any, noise_ref, small_sem.at[0]),
        pltpu.make_async_copy(branches_any, branches_ref, small_sem.at[1]),
    )
    for copy in small:
        copy.start()
    half, quarter, width = users // 2, users // 4, 2 * users
    tail = share * half + quarter
    compact = 2 * symbols <= users
    at, edge8 = iota((half, LANES), 1), iota((quarter, LANES), 1) // users
    even = iota((users, LANES), 1) % 2 == 0
    sends, ready = [], []

    def fold(number, k, products):
        lower = []
        for s, product in enumerate(products):
            slot = (number * share + s) % raw.shape[0]
            raw[slot, :, : width + 2 * symbols] = product
            on_even = raw[slot, pl.ds(0, users, stride=2), :]
            on_odd = raw[slot, pl.ds(1, users, stride=2), :]
            whole = pair_swap(on_odd) + jnp.where(even, on_even, -on_even)
            lower.append(whole[half:])
            upper, bottom = whole[:half], whole[half:]
            if s:
                upper = pltpu.roll(upper, width, 1)
                if compact:
                    upper = jnp.where((at >= users) & (at < width), pltpu.roll(bottom, 3 * users, 1), upper)
            elif compact:
                upper = jnp.where(at < 3 * users, upper, pltpu.roll(bottom, users, 1))
            part[k, s * half : (s + 1) * half] = upper
        part[k, share * half : tail] = jnp.where(
            edge8 == 0, pltpu.roll(lower[1][:quarter], 3 * users, 1),
            jnp.where(
                edge8 == 1, lower[0][quarter:],
                jnp.where(edge8 == 2, pltpu.roll(lower[0][:quarter], users, 1), pltpu.roll(lower[1][quarter:], width, 1)),
            ),
        )
        if not compact:
            part[k, tail:] = jnp.where(at < width, pltpu.roll(lower[0], width, 1), lower[1])
        if k:
            ready.append(
                pltpu.make_async_remote_copy(
                    src_ref=part.at[k], dst_ref=came.at[k], send_sem=send_sem.at[0], recv_sem=recv_sem.at[0],
                    device_id={"chain": peers[k]}, device_id_type=MESH,
                )
            )

    def post(last):
        if ready and (sends or last >= 0):
            if not sends:
                pl.semaphore_wait(barrier, clusters + bands - 2)
            for copy in ready:
                copy.start()
            sends.extend(ready)
            ready.clear()

    raw[...] = jnp.zeros_like(raw)
    waiting = []
    numbered = list(enumerate(order))
    for lot in [numbered[:1]] + [numbered[i : i + 2] for i in range(1, clusters, 2)]:
        fresh = []
        for number, k in lot:
            pltpu.make_async_copy(held.at[k], held.at[k], load_sem.at[k]).wait()
        for number, k in lot:
            products = []
            for s in range(share):
                both = held[k, s]
                products.append(lax.dot_general(both[:width], both, NT, preferred_element_type=jnp.float32))
            fresh.append((number, k, products))
        for chunk in waiting:
            fold(*chunk)
        post(lot[0][0] - 1)
        waiting = fresh
    for chunk in waiting:
        fold(*chunk)
    post(clusters)

    for copy in small:
        copy.wait()
    rows = pieces * mine_t
    source, target = iota((2 * LANES, 4 * LANES), 0), iota((2 * LANES, 4 * LANES), 1)
    place = target % (2 * LANES)
    user, quadrature, off = place // 2, place % 2, target // (2 * LANES)
    entry = jnp.where(source == user + LANES * ((quadrature + off) % 2), 1.0, 0.0)
    entry = jnp.where(off * quadrature == 1, -entry, entry).astype(jnp.bfloat16)
    marks = jnp.concatenate(
        [
            branches_ref[b, s, :, LANES * r : LANES * (r + 1)]
            for b in range(bands) for s in range(share) for r in range(pieces)
        ],
        axis=0,
    )
    pair = jnp.concatenate(
        [(2 * (marks & 7) - 7).astype(jnp.float32), (2 * (marks >> 3) - 7).astype(jnp.float32)], axis=1
    ).astype(jnp.bfloat16)
    woven = jnp.dot(pair, entry, preferred_element_type=jnp.float32).astype(jnp.bfloat16)
    for b in range(bands):
        for s in range(share):
            first = (b * share + s) * rows
            for h in range(2):
                for o in range(2):
                    points[b, s, pl.ds((2 * h + o) * rows, rows), :] = woven[
                        first : first + rows, LANES * (2 * o + h) : LANES * (2 * o + h + 1)
                    ]

    noises = [
        jnp.sum(jnp.where(iota((1, bands), 1) == band, noise_ref[s : s + 1, :], 0.0), axis=1, keepdims=True)
        for s in range(share)
    ]
    row, lanes, extra = iota((8, LANES), 0), iota((8, LANES), 1), 2 * mine_t
    noise = jnp.where(lanes >= width, noises[1], noises[0])
    every = pltpu.make_async_remote_copy(
        src_ref=part.at[pl.ds(1, clusters - 1)], dst_ref=came.at[pl.ds(1, clusters - 1)], send_sem=send_sem.at[0],
        recv_sem=recv_sem.at[0], device_id={"chain": peers[1]}, device_id_type=MESH,
    )
    every.wait_recv()
    total = part[0]
    for k in range(1, clusters):
        total = total + came[k]
    tile, ups = total[share * half : tail], [total[s * half : (s + 1) * half] for s in range(share)]
    inside = iota((quarter, LANES), 1) % width >= users
    above, heard = jnp.where(at < width, ups[0], ups[1]), jnp.where(at < width, ups[1], ups[0])
    below = [jnp.where(inside, x, 0.0) for x in (pltpu.roll(tile, 3 * users, 1), tile)]
    seen = [pltpu.roll(heard, width, 1), pltpu.roll(heard, users, 1) if compact else total[tail:]]
    seen = [jnp.where(at % width < 2 * symbols, x, 0.0) for x in seen]
    lines = [above[:8], above[8:]] + below
    for g in range(users // 8):
        lines[g] = jnp.where(lanes % width == 2 * (row + 8 * g), lines[g] + noise, lines[g])
    upper, rotated = eliminate(lines, [x[8 * i : 8 * i + 8] for x in seen for i in range(half // 8)], users)
    corner = jnp.where(inside, upper[3], pltpu.roll(upper[2], 3 * users, 1))
    for b in range(bands):
        z = jnp.zeros_like(corner)
        for g in range(users // 8):
            slot = (b + g + 1 - users // 8) % (width // extra)
            shift = extra * (slot - b) % LANES
            z = jnp.where(lanes % width // extra == slot, pltpu.roll(rotated[g], shift, 1) if shift else rotated[g], z)
        packed[b, :8] = upper[0]
        packed[b, 8:half] = upper[1]
        packed[b, half : half + quarter] = corner
        packed[b, half + quarter :] = z
    near = []
    inner = jnp.minimum(band, bands - 1 - band)
    outward = jnp.where(2 * band < bands - 1, 1, -1)
    for i in range(1, bands):
        both_sides = (i + 1) // 2 if i % 2 else -(i // 2)
        near.append(band + jnp.where(i <= 2 * inner, both_sides, outward * (i - inner)))
    usends = []
    for i in range(bands - 1, 0, -1):
        peer = near[i - 1]
        copy = pltpu.make_async_remote_copy(
            src_ref=packed.at[peer], dst_ref=taken.at[band], send_sem=usend_sem.at[0], recv_sem=urecv_sem.at[band],
            device_id={"par": peer}, device_id_type=MESH,
        )
        copy.start()
        usends.append(copy)

    r, c = iota((4 * rows, LANES), 0), iota((4 * rows, LANES), 1)
    is_off = (r // rows) % 2
    chosen = jnp.where(c % extra == 2 * (r % mine_t) + is_off, (2 * is_off - 1).astype(jnp.float32), 0.0).astype(jnp.bfloat16)
    slots = [lax.rem(band + g + 1 + (width // extra) - users // 8, width // extra) for g in range(users // 8)]
    sr, sc = iota((width, LANES), 0), iota((width, LANES), 1)
    suffix = [
        jnp.where((sr // users + 2 * h == sc // users) & (sr % users >= sc % users), 1.0 / users, 0.0).astype(jnp.bfloat16)
        for h in range(2)
    ]
    for i in range(bands):
        b = band if i == 0 else near[i - 1]
        if i:
            pltpu.make_async_remote_copy(
                src_ref=packed.at[b], dst_ref=taken.at[b], send_sem=usend_sem.at[0], recv_sem=urecv_sem.at[b],
                device_id={"par": b}, device_id_type=MESH,
            ).wait_recv()
        box = taken if i else packed
        top, corner = box[b, :half], box[b, half : half + quarter]
        straight = [(top, corner, pltpu.roll(corner, users, 1))]
        straight.append((pltpu.roll(top, width, 1), pltpu.roll(corner, width, 1), pltpu.roll(corner, 3 * users, 1)))
        z = box[b, half + quarter :]
        rests = []
        side, edge = iota(top.shape, 1) // width, iota(corner.shape, 1) // users
        for s in range(share):
            weights = []
            for e in range(2):
                above, fourth, third = straight[(s + e) % 2]
                weights += [
                    jnp.where(side == e, above, 0.0),
                    jnp.where(edge == 2 * e + 1, third, 0.0),
                    jnp.where(edge == 2 * e + 1, fourth, 0.0),
                ]
            own = [
                jnp.where(lanes // extra == width * s // extra + slots[g], z, 0.0) for g in range(users // 8)
            ]
            high, low = split(
                jnp.concatenate([jnp.concatenate(weights, axis=0), jnp.concatenate(own + own, axis=0)], axis=1)
            )
            p = jnp.concatenate([points[b, s], chosen], axis=1)
            rest = lax.dot_general(p, high, NT, preferred_element_type=jnp.float32) + lax.dot_general(
                p, low, NT, preferred_element_type=jnp.float32
            )
            rests.append(rest)
        for s, rest in enumerate(rests):
            result = None
            for h in range(2):
                on, off = rest[2 * h * rows : (2 * h + 1) * rows], rest[(2 * h + 1) * rows : (2 * h + 2) * rows]
                for term in split(on * on + off * off):
                    step = jnp.dot(term, suffix[h], preferred_element_type=jnp.float32)
                    result = step if result is None else result + step
            for r in range(pieces):
                out_ref[b, s, :, LANES * r : LANES * (r + 1)] = result[mine_t * r : mine_t * (r + 1)]
    every.wait_send()
    pltpu.make_async_remote_copy(
        src_ref=packed.at[pl.ds(1, bands - 1)], dst_ref=taken.at[pl.ds(1, bands - 1)], send_sem=usend_sem.at[0],
        recv_sem=urecv_sem.at[0], device_id={"par": near[0]}, device_id_type=MESH,
    ).wait_send()


def local(propagation_gains, observed_samples, disturbance_variance, retained_branches):
    clusters, bands = lax.axis_size("chain"), lax.axis_size("par")
    _, tones, double_users, antennas = propagation_gains.shape
    users, symbols = double_users // 2, observed_samples.shape[2] // 2
    share, mine_t = tones // clusters, symbols // bands
    pieces = retained_branches.shape[-1] // LANES
    assert share == 2 and 4 * users == LANES and 4 * mine_t <= users // 2
    dims = (clusters, bands, users, symbols, share, mine_t, pieces)
    lines = share * users // 2 + users // 4 + (0 if 2 * symbols <= users else users // 2)
    f32, bf16 = jnp.float32, jnp.bfloat16
    vmem, dma = pltpu.VMEM, pltpu.SemaphoreType.DMA
    return pl.pallas_call(
        functools.partial(kernel, dims),
        out_shape=pltpu.VMEM(retained_branches.shape, f32),
        in_specs=[
            pl.BlockSpec(memory_space=pl.ANY),
            pl.BlockSpec(memory_space=pl.ANY),
            pl.BlockSpec(memory_space=pl.ANY),
            pl.BlockSpec(memory_space=pl.ANY),
        ],
        out_specs=pl.BlockSpec(memory_space=pltpu.VMEM),
        scratch_shapes=[
            vmem(disturbance_variance.shape[::-1], f32),
            vmem(retained_branches.shape, jnp.int32),
            vmem((clusters, share, 2 * (users + symbols), antennas), bf16),
            vmem((4, 2 * users, LANES), f32),
            vmem((clusters, lines, LANES), f32),
            vmem((clusters, lines, LANES), f32),
            vmem((bands, share, 4 * pieces * mine_t, LANES), bf16),
            vmem((bands, users, LANES), f32),
            vmem((bands, users, LANES), f32),
            dma((2,)), dma((clusters,)), dma((1,)), dma((1,)), dma((1,)), dma((bands,)),
        ],
        compiler_params=pltpu.CompilerParams(collective_id=0, has_side_effects=True),
        name="detect",
    )(*(
        pltpu.with_memory_space_constraint(x, pltpu.HBM)
        for x in (disturbance_variance.T, propagation_gains, observed_samples, retained_branches)
    ))


def solution(mesh):
    placed = (
        P("par", None, None, "chain"),
        P("par", None, None, "chain"),
        P(None, "chain"),
        P(None, "chain", "par", None),
    )
    return jax.shard_map(
        local, mesh=mesh, in_specs=placed, out_specs=P(None, "chain", "par", None), check_vma=False
    )
```

```python
import functools
import jax
import jax.numpy as jnp
from jax import lax
from jax.experimental import pallas as pl
from jax.experimental.pallas import tpu as pltpu
from jax.sharding import PartitionSpec as P

constellation_norm = 1.0 / 42.0**0.5
LANES = 128
MESH = pl.DeviceIdType.MESH
NT = (((1,), (1,)), ((), ()))


def iota(shape, dim):
    return lax.broadcasted_iota(jnp.int32, shape, dim)


def panels(users):
    return [(0, 4), (4, 4)] + [(j, 8) for j in range(8, users, 8)]


def split(x):
    high = x.astype(jnp.bfloat16)
    return high, (x - high.astype(jnp.float32)).astype(jnp.bfloat16)


def pair_swap(x):
    even = iota(x.shape, 1) % 2 == 0
    return jnp.where(even, pltpu.roll(x, LANES - 1, 1), pltpu.roll(x, 1, 1))


def eliminate(a, q, users):
    groups, width = users // 8, 2 * users
    row, lanes = iota((8, LANES), 0), iota((8, LANES), 1)
    tone = jnp.where(lanes >= width, width, 0)
    ia, iq = [[jnp.where(lanes % 2 == 1, pair_swap(p), -pair_swap(p)) for p in x] for x in (a, q)]
    by_row = [jnp.ones((8, LANES), jnp.float32) for _ in range(groups)]
    for start, size in panels(users):
        home = start // 8
        panel = []
        for j in range(start, start + size):
            pivot = jnp.broadcast_to(a[home][j % 8 : j % 8 + 1, :], (8, LANES))
            for c in range(2):
                found = {}
                for g in range(home, groups):
                    if start < users // 2 <= 8 * g:
                        ones = [
                            jnp.sum(jnp.where(lanes == t * width + 2 * (row + 8 * g) + c, pivot, 0.0), axis=1, keepdims=True)
                            for t in range(2)
                        ]
                        found[g] = jnp.where(lanes >= width, ones[1], ones[0])
                        if c:
                            found[g] = -found[g]
                    else:
                        found[g] = jnp.take_along_axis(a[g], tone + (2 * j + c), axis=1, mode="promise_in_bounds")
                panel.append(found)
        for j in range(start, start + size):
            at, c = j % 8, j - start
            real, imag = panel[2 * c], panel[2 * c + 1]
            top = real[home][at : at + 1, :]
            by_row[home] = jnp.where(row == at, lax.rsqrt(top), by_row[home])
            if j == users - 1:
                break
            inverse = 1.0 / top
            pivots = [(x, ix, x[home][at : at + 1, :] * inverse, ix[home][at : at + 1, :] * inverse) for x, ix in ((a, ia), (q, iq))]
            later = [
                (d, real[home][at + d - c : at + d - c + 1, :] * inverse, imag[home][at + d - c : at + d - c + 1, :] * inverse)
                for d in range(c + 1, size)
            ]
            for g in range(home + (at == 7), groups):
                fr, fi = real[g], imag[g]
                if g == home:
                    fr, fi = jnp.where(row > at, fr, 0.0), jnp.where(row > at, fi, 0.0)
                for d, x, y in later:
                    panel[2 * d][g] = panel[2 * d][g] - (fr * x + fi * y)
                    panel[2 * d + 1][g] = panel[2 * d + 1][g] - (fi * x - fr * y)
                for x, ix, pivot_row, turned_row in pivots:
                    x[g] = x[g] - (fr * pivot_row + fi * turned_row)
                    ix[g] = ix[g] - (fr * turned_row - fi * pivot_row)
    upper = []
    for g in range(groups):
        diagonal = 2 * (row + 8 * g)
        keep = (lanes % width >= diagonal) & (lanes % width != diagonal + 1)
        upper.append(jnp.where(keep, a[g] * (by_row[g] * constellation_norm), 0.0))
    return upper, [x * scale for x, scale in zip(q, by_row)]


def kernel(
    dims, noise_any, gains_ref, samples_ref, branches_any, out_ref,
    noise_ref, branches_ref, held, raw, part, came, points, packed, taken,
    small_sem, load_sem, send_sem, recv_sem, urecv_sem,
):
    clusters, bands, users, symbols, share, mine_t, pieces = dims
    me, band = lax.axis_index("chain"), lax.axis_index("par")

    far, mid = clusters // 2, clusters // 4
    order = list(range(clusters - 1, -1, -1))
    peers = {}
    for k in order:
        peers[k], bit = me - me, 1
        while bit < clusters:
            digit = lax.rem(me // bit, 2)
            peers[k] = peers[k] + bit * (1 - digit if (k // bit) % 2 else digit)
            bit *= 2
    def load(k):
        tones = pl.ds(peers[k] * share, share)
        pltpu.make_async_copy(gains_ref.at[0, tones], held.at[k, :, pl.ds(0, 2 * users)], load_sem.at[(k + 1) // 2]).start()
        pltpu.make_async_copy(
            samples_ref.at[0, tones], held.at[k, :, pl.ds(2 * users, 2 * symbols)], load_sem.at[(k + 1) // 2]
        ).start()

    for k in order[:clusters]:
        load(k)
    barrier = pltpu.get_barrier_semaphore()
    for k in range(1, clusters):
        pl.semaphore_signal(barrier, inc=1, device_id={"chain": lax.rem(me + k, clusters)}, device_id_type=MESH)
    for k in range(1, bands):
        pl.semaphore_signal(barrier, inc=1, device_id={"par": lax.rem(band + k, bands)}, device_id_type=MESH)

    small = (
        pltpu.make_async_copy(noise_any, noise_ref, small_sem.at[0]),
        pltpu.make_async_copy(branches_any, branches_ref, small_sem.at[1]),
    )
    for copy in small:
        copy.start()
    half, quarter, width = users // 2, users // 4, 2 * users
    tail = share * half + quarter
    compact = 2 * symbols <= users
    at, edge8 = iota((half, LANES), 1), iota((quarter, LANES), 1) // users
    even = iota((users, LANES), 1) % 2 == 0
    sends, ready = [], []

    def fold(number, k, products):
        lower = []
        for s, product in enumerate(products):
            slot = (number * share + s) % raw.shape[0]
            raw[slot, :, : width + 2 * symbols] = product
            on_even = raw[slot, pl.ds(0, users, stride=2), :]
            on_odd = raw[slot, pl.ds(1, users, stride=2), :]
            whole = pair_swap(on_odd) + jnp.where(even, on_even, -on_even)
            lower.append(whole[half:])
            upper, bottom = whole[:half], whole[half:]
            if s:
                upper = pltpu.roll(upper, width, 1)
                if compact:
                    upper = jnp.where((at >= users) & (at < width), pltpu.roll(bottom, 3 * users, 1), upper)
            elif compact:
                upper = jnp.where(at < 3 * users, upper, pltpu.roll(bottom, users, 1))
            part[k, s * half : (s + 1) * half] = upper
        part[k, share * half : tail] = jnp.where(
            edge8 == 0, pltpu.roll(lower[1][:quarter], 3 * users, 1),
            jnp.where(
                edge8 == 1, lower[0][quarter:],
                jnp.where(edge8 == 2, pltpu.roll(lower[0][:quarter], users, 1), pltpu.roll(lower[1][quarter:], width, 1)),
            ),
        )
        if not compact:
            part[k, tail:] = jnp.where(at < width, pltpu.roll(lower[0], width, 1), lower[1])
        if k:
            ready.append(
                pltpu.make_async_remote_copy(
                    src_ref=part.at[k], dst_ref=came.at[k], send_sem=send_sem.at[0], recv_sem=recv_sem.at[0],
                    device_id={"chain": peers[k]}, device_id_type=MESH,
                )
            )

    def post(last):
        if ready and (sends or last >= 0):
            if not sends:
                pl.semaphore_wait(barrier, clusters + bands - 2)
            for copy in ready:
                copy.start()
            sends.extend(ready)
            ready.clear()

    raw[...] = jnp.zeros_like(raw)
    waiting = []
    numbered = list(enumerate(order))
    for lot in [numbered[:1]] + [numbered[i : i + 2] for i in range(1, clusters, 2)]:
        fresh = []
        landed = held.at[pl.ds(lot[-1][1], len(lot))]
        pltpu.make_async_copy(landed, landed, load_sem.at[(lot[0][1] + 1) // 2]).wait()
        for number, k in lot:
            products = []
            for s in range(share):
                both = held[k, s]
                products.append(lax.dot_general(both[:width], both, NT, preferred_element_type=jnp.float32))
            fresh.append((number, k, products))
        for chunk in waiting:
            fold(*chunk)
        post(lot[0][0] - 1)
        waiting = fresh
    for chunk in waiting:
        fold(*chunk)
    post(clusters)

    for copy in small:
        copy.wait()
    rows = pieces * mine_t
    source, target = iota((2 * LANES, 4 * LANES), 0), iota((2 * LANES, 4 * LANES), 1)
    place = target % (2 * LANES)
    user, quadrature, off = place // 2, place % 2, target // (2 * LANES)
    entry = jnp.where(source == user + LANES * ((quadrature + off) % 2), 1.0, 0.0)
    entry = jnp.where(off * quadrature == 1, -entry, entry).astype(jnp.bfloat16)
    marks = jnp.concatenate(
        [
            branches_ref[b, s, :, LANES * r : LANES * (r + 1)]
            for b in range(bands) for s in range(share) for r in range(pieces)
        ],
        axis=0,
    )
    pair = jnp.concatenate(
        [(2 * (marks & 7) - 7).astype(jnp.float32), (2 * (marks >> 3) - 7).astype(jnp.float32)], axis=1
    ).astype(jnp.bfloat16)
    woven = jnp.dot(pair, entry, preferred_element_type=jnp.float32).astype(jnp.bfloat16)
    for b in range(bands):
        for s in range(share):
            first = (b * share + s) * rows
            for h in range(2):
                for o in range(2):
                    points[b, s, pl.ds((2 * h + o) * rows, rows), :] = woven[
                        first : first + rows, LANES * (2 * o + h) : LANES * (2 * o + h + 1)
                    ]

    noises = [
        jnp.sum(jnp.where(iota((1, bands), 1) == band, noise_ref[s : s + 1, :], 0.0), axis=1, keepdims=True)
        for s in range(share)
    ]
    row, lanes, extra = iota((8, LANES), 0), iota((8, LANES), 1), 2 * mine_t
    noise = jnp.where(lanes >= width, noises[1], noises[0])
    every = pltpu.make_async_remote_copy(
        src_ref=part.at[pl.ds(1, clusters - 1)], dst_ref=came.at[pl.ds(1, clusters - 1)], send_sem=send_sem.at[0],
        recv_sem=recv_sem.at[0], device_id={"chain": peers[1]}, device_id_type=MESH,
    )
    every.wait_recv()
    total = part[0]
    for k in range(1, clusters):
        total = total + came[k]
    tile, ups = total[share * half : tail], [total[s * half : (s + 1) * half] for s in range(share)]
    inside = iota((quarter, LANES), 1) % width >= users
    above, heard = jnp.where(at < width, ups[0], ups[1]), jnp.where(at < width, ups[1], ups[0])
    below = [jnp.where(inside, x, 0.0) for x in (pltpu.roll(tile, 3 * users, 1), tile)]
    seen = [pltpu.roll(heard, width, 1), pltpu.roll(heard, users, 1) if compact else total[tail:]]
    seen = [jnp.where(at % width < 2 * symbols, x, 0.0) for x in seen]
    lines = [above[:8], above[8:]] + below
    for g in range(users // 8):
        lines[g] = jnp.where(lanes % width == 2 * (row + 8 * g), lines[g] + noise, lines[g])
    upper, rotated = eliminate(lines, [x[8 * i : 8 * i + 8] for x in seen for i in range(half // 8)], users)
    corner = jnp.where(inside, upper[3], pltpu.roll(upper[2], 3 * users, 1))
    for b in range(bands):
        z = jnp.zeros_like(corner)
        for g in range(users // 8):
            slot = (b + g + 1 - users // 8) % (width // extra)
            shift = extra * (slot - b) % LANES
            z = jnp.where(lanes % width // extra == slot, pltpu.roll(rotated[g], shift, 1) if shift else rotated[g], z)
        packed[b, :8] = upper[0]
        packed[b, 8:half] = upper[1]
        packed[b, half : half + quarter] = corner
        packed[b, half + quarter :] = z
    near = []
    inner = jnp.minimum(band, bands - 1 - band)
    outward = jnp.where(2 * band < bands - 1, 1, -1)
    for i in range(1, bands):
        both_sides = (i + 1) // 2 if i % 2 else -(i // 2)
        near.append(band + jnp.where(i <= 2 * inner, both_sides, outward * (i - inner)))
    usends = []
    for i in range(bands - 1, 0, -1):
        peer = near[i - 1]
        copy = pltpu.make_async_remote_copy(
            src_ref=packed.at[peer], dst_ref=taken.at[band], send_sem=load_sem.at[0], recv_sem=urecv_sem.at[band],
            device_id={"par": peer}, device_id_type=MESH,
        )
        copy.start()
        usends.append(copy)

    r, c = iota((4 * rows, LANES), 0), iota((4 * rows, LANES), 1)
    is_off = (r // rows) % 2
    chosen = jnp.where(c % extra == 2 * (r % mine_t) + is_off, (2 * is_off - 1).astype(jnp.float32), 0.0).astype(jnp.bfloat16)
    slots = [lax.rem(band + g + 1 + (width // extra) - users // 8, width // extra) for g in range(users // 8)]
    sr, sc = iota((width, LANES), 0), iota((width, LANES), 1)
    suffix = [
        jnp.where((sr // users + 2 * h == sc // users) & (sr % users >= sc % users), 1.0 / users, 0.0).astype(jnp.bfloat16)
        for h in range(2)
    ]
    for i in range(bands):
        b = band if i == 0 else near[i - 1]
        if i:
            pltpu.make_async_remote_copy(
                src_ref=packed.at[b], dst_ref=taken.at[b], send_sem=load_sem.at[0], recv_sem=urecv_sem.at[b],
                device_id={"par": b}, device_id_type=MESH,
            ).wait_recv()
        box = taken if i else packed
        top, corner = box[b, :half], box[b, half : half + quarter]
        straight = [(top, corner, pltpu.roll(corner, users, 1))]
        straight.append((pltpu.roll(top, width, 1), pltpu.roll(corner, width, 1), pltpu.roll(corner, 3 * users, 1)))
        z = box[b, half + quarter :]
        rests = []
        side, edge = iota(top.shape, 1) // width, iota(corner.shape, 1) // users
        for s in range(share):
            weights = []
            for e in range(2):
                above, fourth, third = straight[(s + e) % 2]
                weights += [
                    jnp.where(side == e, above, 0.0),
                    jnp.where(edge == 2 * e + 1, third, 0.0),
                    jnp.where(edge == 2 * e + 1, fourth, 0.0),
                ]
            own = [
                jnp.where(lanes // extra == width * s // extra + slots[g], z, 0.0) for g in range(users // 8)
            ]
            high, low = split(
                jnp.concatenate([jnp.concatenate(weights, axis=0), jnp.concatenate(own + own, axis=0)], axis=1)
            )
            p = jnp.concatenate([points[b, s], chosen], axis=1)
            rest = lax.dot_general(p, high, NT, preferred_element_type=jnp.float32) + lax.dot_general(
                p, low, NT, preferred_element_type=jnp.float32
            )
            rests.append(rest)
        for s, rest in enumerate(rests):
            result = None
            for h in range(2):
                on, off = rest[2 * h * rows : (2 * h + 1) * rows], rest[(2 * h + 1) * rows : (2 * h + 2) * rows]
                for term in split(on * on + off * off):
                    step = jnp.dot(term, suffix[h], preferred_element_type=jnp.float32)
                    result = step if result is None else result + step
            for r in range(pieces):
                out_ref[b, s, :, LANES * r : LANES * (r + 1)] = result[mine_t * r : mine_t * (r + 1)]
    every.wait_send()
    pltpu.make_async_remote_copy(
        src_ref=packed.at[pl.ds(1, bands - 1)], dst_ref=taken.at[pl.ds(1, bands - 1)], send_sem=load_sem.at[0],
        recv_sem=urecv_sem.at[0], device_id={"par": near[0]}, device_id_type=MESH,
    ).wait_send()


def local(propagation_gains, observed_samples, disturbance_variance, retained_branches):
    clusters, bands = lax.axis_size("chain"), lax.axis_size("par")
    _, tones, double_users, antennas = propagation_gains.shape
    users, symbols = double_users // 2, observed_samples.shape[2] // 2
    share, mine_t = tones // clusters, symbols // bands
    pieces = retained_branches.shape[-1] // LANES
    assert share == 2 and 4 * users == LANES and 4 * mine_t <= users // 2
    dims = (clusters, bands, users, symbols, share, mine_t, pieces)
    lines = share * users // 2 + users // 4 + (0 if 2 * symbols <= users else users // 2)
    f32, bf16 = jnp.float32, jnp.bfloat16
    vmem, dma = pltpu.VMEM, pltpu.SemaphoreType.DMA
    return pl.pallas_call(
        functools.partial(kernel, dims),
        out_shape=pltpu.VMEM(retained_branches.shape, f32),
        in_specs=[
            pl.BlockSpec(memory_space=pl.ANY),
            pl.BlockSpec(memory_space=pl.ANY),
            pl.BlockSpec(memory_space=pl.ANY),
            pl.BlockSpec(memory_space=pl.ANY),
        ],
        out_specs=pl.BlockSpec(memory_space=pltpu.VMEM),
        scratch_shapes=[
            vmem(disturbance_variance.shape[::-1], f32),
            vmem(retained_branches.shape, jnp.int32),
            vmem((clusters, share, 2 * (users + symbols), antennas), bf16),
            vmem((4, 2 * users, LANES), f32),
            vmem((clusters, lines, LANES), f32),
            vmem((clusters, lines, LANES), f32),
            vmem((bands, share, 4 * pieces * mine_t, LANES), bf16),
            vmem((bands, users, LANES), f32),
            vmem((bands, users, LANES), f32),
            dma((2,)), dma((clusters // 2 + 1,)), dma((1,)), dma((1,)), dma((bands,)),
        ],
        compiler_params=pltpu.CompilerParams(collective_id=0, has_side_effects=True),
        name="detect",
    )(*(
        pltpu.with_memory_space_constraint(x, pltpu.HBM)
        for x in (disturbance_variance.T, propagation_gains, observed_samples, retained_branches)
    ))


def solution(mesh):
    placed = (
        P("par", None, None, "chain"),
        P("par", None, None, "chain"),
        P(None, "chain"),
        P(None, "chain", "par", None),
    )
    return jax.shard_map(
        local, mesh=mesh, in_specs=placed, out_specs=P(None, "chain", "par", None), check_vma=False
    )
```
